32 devices in a mesh: dp: 2 (over x), tp: 16 (over z, y, core).
Axes of the slice: x: 2, y: 2, z: 4, core: 2. Of those that a mesh axis runs over, the one named last changes fastest.
Arguments:
- x_steps: bfloat16 [16, 128, 4096], P(None, 'dp'), parts along dimension 1
- cur_len: int32 [128], P('dp'), parts along dimension 0
- k_cache: bfloat16 [2, 128, 64, 16, 256], P(None, 'dp', None, 'tp'), parts along dimension 1
- v_cache: bfloat16 [2, 128, 64, 16, 256], P(None, 'dp', None, 'tp'), parts along dimension 1
- ln_gain: bfloat16 [2, 4096], replicated
- ln_bias: bfloat16 [2, 4096], replicated
- w_q: bfloat16 [2, 4096, 4096], P(None, None, 'tp')
- w_k: bfloat16 [2, 4096, 4096], P(None, None, 'tp')
- w_v: bfloat16 [2, 4096, 4096], P(None, None, 'tp')
- w_o: bfloat16 [2, 4096, 4096], P(None, 'tp')
- w_in: bfloat16 [2, 4096, 16384], P(None, None, 'tp')
- b_in: bfloat16 [2, 16384], P(None, 'tp')
- w_out: bfloat16 [2, 16384, 4096], P(None, 'tp')
- b_out: bfloat16 [2, 4096], replicated
Outputs:
- output 1: bfloat16 [16, 128, 4096], P(None, 'dp'), parts along dimension 1
- output 2: bfloat16 [2, 128, 64, 16, 256], P(None, 'dp', None, 'tp'), parts along dimension 1
- output 3: bfloat16 [2, 128, 64, 16, 256], P(None, 'dp', None, 'tp'), parts along dimension 1
There are 2 independent parts. The reference program is written for one: setup_inputs(seed, part) draws one part's arguments, and reference() takes and returns one part's arrays. A program takes and returns all parts, laid end to end along the dimension named above; an argument that names none is the same for every part.
All inputs are finite; a program needn't handle non-finite values.
Results may differ from the reference program's by a relative error of at most 0.0176966.
Values are sent between devices in bfloat16 or wider.
A program may use at most 1 GiB of HBM per device.

```python
import jax
import jax.numpy as jnp
from jax import lax

D_MODEL = 4096
N_HEADS = 16
HEAD_DIM = 256
ROT_DIM = 64
FF_DIM = 16384
BATCH_PART = 64
CACHE_LEN = 64
N_STEPS = 16
N_LAYERS = 2
LN_EPS = 1e-5
QUERY_GAIN = 2.5


def setup_inputs(seed: int = 0, part: int = 0) -> dict:
    base_key = jax.random.key(seed)
    shared_keys = jax.random.split(base_key, 10)
    part_keys = jax.random.split(jax.random.fold_in(base_key, part), 6)
    scale_model = D_MODEL ** -0.5
    scale_ff = FF_DIM ** -0.5
    cache_shape = (N_LAYERS, BATCH_PART, CACHE_LEN, N_HEADS, HEAD_DIM)

    def gaussian(key, shape, scale):
        return jax.random.normal(key, shape, jnp.float32) * scale

    top_len = CACHE_LEN - N_STEPS
    raw_span = jax.random.randint(part_keys[1], (BATCH_PART,), 0, top_len)
    shift_bits = jax.random.randint(part_keys[2], (BATCH_PART,), 0, 8)
    full_row = jax.random.randint(part_keys[3], (), 0, BATCH_PART)
    cur_len = 1 + jnp.right_shift(raw_span, shift_bits)
    cur_len = jnp.where(jnp.arange(BATCH_PART) == full_row, top_len, cur_len).astype(jnp.int32)
    return {
        "x_steps": gaussian(part_keys[0], (N_STEPS, BATCH_PART, D_MODEL), 1.0).astype(jnp.bfloat16),
        "cur_len": cur_len,
        "k_cache": gaussian(part_keys[4], cache_shape, 1.0).astype(jnp.bfloat16),
        "v_cache": gaussian(part_keys[5], cache_shape, 1.0).astype(jnp.bfloat16),
        "ln_gain": (1.0 + gaussian(shared_keys[0], (N_LAYERS, D_MODEL), 0.2)).astype(jnp.bfloat16),
        "ln_bias": gaussian(shared_keys[1], (N_LAYERS, D_MODEL), 0.2).astype(jnp.bfloat16),
        "w_q": gaussian(shared_keys[2], (N_LAYERS, D_MODEL, D_MODEL), QUERY_GAIN * scale_model).astype(jnp.bfloat16),
        "w_k": gaussian(shared_keys[3], (N_LAYERS, D_MODEL, D_MODEL), scale_model).astype(jnp.bfloat16),
        "w_v": gaussian(shared_keys[4], (N_LAYERS, D_MODEL, D_MODEL), scale_model).astype(jnp.bfloat16),
        "w_o": gaussian(shared_keys[5], (N_LAYERS, D_MODEL, D_MODEL), scale_model).astype(jnp.bfloat16),
        "w_in": gaussian(shared_keys[6], (N_LAYERS, D_MODEL, FF_DIM), scale_model).astype(jnp.bfloat16),
        "b_in": gaussian(shared_keys[7], (N_LAYERS, FF_DIM), 0.5).astype(jnp.bfloat16),
        "w_out": gaussian(shared_keys[8], (N_LAYERS, FF_DIM, D_MODEL), scale_ff).astype(jnp.bfloat16),
        "b_out": gaussian(shared_keys[9], (N_LAYERS, D_MODEL), 0.3).astype(jnp.bfloat16),
    }


def layer_norm(hidden, gain, bias):
    hid_f32 = hidden.astype(jnp.float32)
    row_mean = jnp.mean(hid_f32, axis=-1, keepdims=True)
    centered = hid_f32 - row_mean
    row_var = jnp.mean(centered * centered, axis=-1, keepdims=True)
    normed = centered / jnp.sqrt(row_var + LN_EPS)
    return (normed * gain.astype(jnp.float32) + bias.astype(jnp.float32)).astype(jnp.bfloat16)


def rotary_tables(positions):
    inv_freq = 1.0 / (10000.0 ** (jnp.arange(0, ROT_DIM, 2).astype(jnp.float32) / ROT_DIM))
    angles = positions.astype(jnp.float32)[:, None] * inv_freq[None, :]
    return jnp.cos(angles)[:, None, :], jnp.sin(angles)[:, None, :]


def apply_rotary(vectors, cos_tab, sin_tab):
    lead_shape = vectors.shape[:-1]
    pairs = vectors[..., :ROT_DIM].reshape(lead_shape + (ROT_DIM // 2, 2))
    even_part = pairs[..., 0]
    odd_part = pairs[..., 1]
    rotated = jnp.stack([even_part * cos_tab - odd_part * sin_tab, odd_part * cos_tab + even_part * sin_tab], axis=-1)
    return jnp.concatenate([rotated.reshape(lead_shape + (ROT_DIM,)), vectors[..., ROT_DIM:]], axis=-1)


def decoder_layer(hidden, new_pos, layer):
    (k_layer, v_layer, gain, bias, q_weight, k_weight, v_weight, o_weight,
     in_weight, in_bias, out_weight, out_bias) = layer
    batch = hidden.shape[0]
    head_shape = (batch, N_HEADS, HEAD_DIM)
    normed = layer_norm(hidden, gain, bias)
    query = jnp.dot(normed, q_weight, preferred_element_type=jnp.float32).reshape(head_shape)
    key_new = jnp.dot(normed, k_weight, preferred_element_type=jnp.float32).reshape(head_shape)
    value_new = jnp.dot(normed, v_weight, preferred_element_type=jnp.float32).reshape(head_shape).astype(jnp.bfloat16)
    cos_tab, sin_tab = rotary_tables(new_pos)
    query = apply_rotary(query, cos_tab, sin_tab).astype(jnp.bfloat16)
    key_new = apply_rotary(key_new, cos_tab, sin_tab).astype(jnp.bfloat16)
    slot_ids = jnp.arange(CACHE_LEN)
    written = (slot_ids[None, :] == new_pos[:, None])[:, :, None, None]
    k_layer = jnp.where(written, key_new[:, None], k_layer)
    v_layer = jnp.where(written, value_new[:, None], v_layer)
    scores = jnp.einsum("bhe,bshe->bhs", query.astype(jnp.float32), k_layer.astype(jnp.float32)) * (HEAD_DIM ** -0.5)
    visible = (slot_ids[None, :] <= new_pos[:, None])[:, None, :]
    scores = jnp.where(visible, scores, -jnp.inf)
    exp_scores = jnp.exp(scores - jnp.max(scores, axis=-1, keepdims=True))
    attn_probs = (exp_scores / jnp.sum(exp_scores, axis=-1, keepdims=True)).astype(jnp.bfloat16)
    context = jnp.einsum("bhs,bshe->bhe", attn_probs.astype(jnp.float32), v_layer.astype(jnp.float32))
    context = context.astype(jnp.bfloat16).reshape(batch, N_HEADS * HEAD_DIM)
    attn_out = jnp.dot(context, o_weight, preferred_element_type=jnp.float32)
    pre_act = jnp.dot(normed, in_weight, preferred_element_type=jnp.float32) + in_bias.astype(jnp.float32)
    gelu_act = jax.nn.gelu(pre_act, approximate=True).astype(jnp.bfloat16)
    mlp_out = jnp.dot(gelu_act, out_weight, preferred_element_type=jnp.float32)
    new_hidden = (hidden.astype(jnp.float32) + attn_out + mlp_out + out_bias.astype(jnp.float32)).astype(jnp.bfloat16)
    return new_hidden, (k_layer, v_layer)


def reference(x_steps, cur_len, k_cache, v_cache, ln_gain, ln_bias, w_q, w_k, w_v, w_o, w_in, b_in, w_out, b_out):
    def one_step(caches, step_in):
        x_now, step_idx = step_in
        new_pos = cur_len + step_idx

        def layer_step(hidden, layer):
            return decoder_layer(hidden, new_pos, layer)

        layers = (caches[0], caches[1], ln_gain, ln_bias, w_q, w_k, w_v, w_o, w_in, b_in, w_out, b_out)
        last_hidden, new_caches = lax.scan(layer_step, x_now, layers)
        return new_caches, last_hidden

    final_caches, hidden_out = lax.scan(one_step, (k_cache, v_cache), (x_steps, jnp.arange(N_STEPS, dtype=jnp.int32)))
    return hidden_out, final_caches[0], final_caches[1]
```

```python
import jax
import jax.numpy as jnp
from jax import lax
from jax.sharding import PartitionSpec as P

ROT_DIM = 64
LN_EPS = 1e-5
TP = 16
CHUNKS = 2


def layer_norm(hidden, gain, bias):
    hid_f32 = hidden.astype(jnp.float32)
    row_mean = jnp.mean(hid_f32, axis=-1, keepdims=True)
    centered = hid_f32 - row_mean
    row_var = jnp.mean(centered * centered, axis=-1, keepdims=True)
    normed = centered * lax.rsqrt(row_var + LN_EPS)
    return (normed * gain.astype(jnp.float32) + bias.astype(jnp.float32)).astype(jnp.bfloat16)


def rotary_full(positions, width):
    inv_freq = 1.0 / (10000.0 ** (jnp.arange(0, ROT_DIM, 2).astype(jnp.float32) / ROT_DIM))
    angles = positions.astype(jnp.float32)[:, None] * inv_freq[None, :]
    cos = jnp.repeat(jnp.cos(angles), 2, axis=1)
    sin = jnp.repeat(jnp.sin(angles), 2, axis=1) * jnp.where(jnp.arange(ROT_DIM) % 2 == 0, -1.0, 1.0)
    rest = width - ROT_DIM
    return jnp.pad(cos, ((0, 0), (0, rest)), constant_values=1.0), jnp.pad(sin, ((0, 0), (0, rest)))


def rotate(vec, cos, sin):
    even = jnp.arange(vec.shape[1]) % 2 == 0
    swapped = jnp.where(even, jnp.roll(vec, -1, axis=1), jnp.roll(vec, 1, axis=1))
    return vec * cos + swapped * sin


def write_slots(cache, new, first):
    steps = jnp.arange(new.shape[0])
    offset = jnp.arange(cache.shape[1])[None, :] - first[:, None]
    one_hot = (offset[:, :, None] == steps).astype(jnp.bfloat16)
    placed = jnp.einsum("bst,tbe->bse", one_hot, new, preferred_element_type=jnp.float32).astype(jnp.bfloat16)
    written = (offset >= 0) & (offset < new.shape[0])
    return jnp.where(written[:, :, None], placed, cache)


def layer_update(normed, cos, sin, cur_len, first_step, k_cache, v_cache, weights):
    w_q, w_k, w_v, w_o, w_in, b_in, w_out = weights
    batch, slots, dim = k_cache.shape
    steps = normed.shape[0] // batch
    query = rotate(jnp.dot(normed, w_q, preferred_element_type=jnp.float32), cos, sin).astype(jnp.bfloat16)
    key = rotate(jnp.dot(normed, w_k, preferred_element_type=jnp.float32), cos, sin).astype(jnp.bfloat16)
    value = jnp.dot(normed, w_v, preferred_element_type=jnp.float32).astype(jnp.bfloat16)
    first = cur_len + first_step
    k_cache = write_slots(k_cache, key.reshape(steps, batch, dim), first)
    v_cache = write_slots(v_cache, value.reshape(steps, batch, dim), first)
    scores = jnp.einsum("tbe,bse->bts", query.reshape(steps, batch, dim), k_cache, preferred_element_type=jnp.float32) * (dim ** -0.5)
    visible = jnp.arange(slots) <= (first[:, None] + jnp.arange(steps))[:, :, None]
    scores = jnp.where(visible, scores, -jnp.inf)
    exp_scores = jnp.exp(scores - jnp.max(scores, axis=-1, keepdims=True))
    probs = (exp_scores / jnp.sum(exp_scores, axis=-1, keepdims=True)).astype(jnp.bfloat16)
    context = jnp.einsum("bts,bse->tbe", probs, v_cache, preferred_element_type=jnp.float32)
    context = context.astype(jnp.bfloat16).reshape(steps * batch, dim)
    pre_act = jnp.dot(normed, w_in, preferred_element_type=jnp.float32) + b_in.astype(jnp.float32)
    act = jax.nn.gelu(pre_act, approximate=True).astype(jnp.bfloat16)
    part = jnp.dot(context, w_o, preferred_element_type=jnp.float32) + jnp.dot(act, w_out, preferred_element_type=jnp.float32)
    return part.astype(jnp.bfloat16), k_cache, v_cache


def decode_shard(x_steps, cur_len, k_cache, v_cache, ln_gain, ln_bias, w_q, w_k, w_v, w_o, w_in, b_in, w_out, b_out):
    n_layers, batch, slots, _, dim = k_cache.shape
    total, _, width = x_steps.shape
    steps = total // CHUNKS
    rows = steps * batch
    own = rows // TP
    me = lax.axis_index("tp")
    k_caches = [k_cache[layer, :, :, 0] for layer in range(n_layers)]
    v_caches = [v_cache[layer, :, :, 0] for layer in range(n_layers)]
    xs = [x_steps[c * steps:(c + 1) * steps].reshape(rows, width) for c in range(CHUNKS)]
    normed = [layer_norm(x, ln_gain[0], ln_bias[0]) for x in xs]
    hidden = [lax.dynamic_slice_in_dim(x, me * own, own) for x in xs]
    tables = []
    for c in range(CHUNKS):
        pos = (cur_len[None, :] + (c * steps + jnp.arange(steps))[:, None]).reshape(rows)
        tables.append(rotary_full(pos, dim))
    outputs = []
    for layer in range(n_layers):
        weights = (w_q[layer], w_k[layer], w_v[layer], w_o[layer], w_in[layer], b_in[layer], w_out[layer])
        for c in range(CHUNKS):
            cos, sin = tables[c]
            part, k_caches[layer], v_caches[layer] = layer_update(
                normed[c], cos, sin, cur_len, c * steps, k_caches[layer], v_caches[layer], weights)
            mine = lax.psum_scatter(part, "tp", scatter_dimension=0, tiled=True)
            hidden[c] = (hidden[c].astype(jnp.float32) + mine.astype(jnp.float32) + b_out[layer].astype(jnp.float32)).astype(jnp.bfloat16)
            if layer + 1 < n_layers:
                send = layer_norm(hidden[c], ln_gain[layer + 1], ln_bias[layer + 1])
                normed[c] = lax.all_gather(send, "tp", axis=0, tiled=True)
            else:
                outputs.append(lax.all_gather(hidden[c], "tp", axis=0, tiled=True).reshape(steps, batch, width))
    return jnp.concatenate(outputs), jnp.stack(k_caches)[:, :, :, None], jnp.stack(v_caches)[:, :, :, None]


def solution(mesh):
    cache_spec = P(None, "dp", None, "tp", None)
    in_specs = (P(None, "dp", None), P("dp"), cache_spec, cache_spec, P(None, None), P(None, None),
                P(None, None, "tp"), P(None, None, "tp"), P(None, None, "tp"), P(None, "tp", None),
                P(None, None, "tp"), P(None, "tp"), P(None, "tp", None), P(None, None))
    out_specs = (P(None, "dp", None), cache_spec, cache_spec)
    return jax.shard_map(decode_shard, mesh=mesh, in_specs=in_specs, out_specs=out_specs, check_vma=False)
```

```python
import functools

import jax
import jax.numpy as jnp
from jax import lax
from jax.experimental import pallas as pl
from jax.experimental.pallas import tpu as pltpu
from jax.sharding import PartitionSpec as P

ROT_DIM = 64
LN_EPS = 1e-5
TP = 16
CHIPS = 8
STREAMS = 4
BF16 = jnp.bfloat16
F32 = jnp.float32
VMEM_LIMIT = 67_000_000
SLOT = {0: 0, -1: 1, 1: 2, -2: 3, 2: 4, -3: 5, 3: 6, 4: 7, -4: 7}
OFFSETS = (0, -1, 1, -2, 2, -3, 3, 4)


def ring_of_chip(chip):
    z, y = lax.div(chip, 2), lax.rem(chip, 2)
    return z + y * (7 - 2 * z)


def chip_of_ring(pos):
    pos = lax.rem(pos + 2 * CHIPS, CHIPS)
    y = lax.div(pos, 4)
    z = pos + y * (7 - 2 * pos)
    return 2 * z + y


def norm_rows(x, gain, bias):
    mean = jnp.mean(x, axis=-1, keepdims=True)
    centered = x - mean
    var = jnp.mean(centered * centered, axis=-1, keepdims=True)
    return (centered * lax.rsqrt(var + LN_EPS) * gain + bias).astype(BF16)


def rotate(vec, cos, sin):
    head, rest = vec[:, :128], vec[:, 128:]
    even = lax.rem(lax.broadcasted_iota(jnp.int32, head.shape, 1), 2) == 0
    swapped = jnp.where(even, pltpu.roll(head, 127, 1), pltpu.roll(head, 1, 1))
    return jnp.concatenate([head * cos + swapped * sin, rest], axis=1).astype(BF16)


def project(lhs_piece, rows, cos_of, sin_of, w_qkv, w_in, b_in_of, qkv_out, act_out):
    def product(w_ref_cols):
        total = None
        for i in range(STREAMS):
            lhs = lhs_piece(i)
            depth = lhs.shape[1]
            term = jnp.dot(lhs, w_ref_cols(i * depth, depth), preferred_element_type=F32)
            total = term if total is None else total + term
        return total

    def put(ref, index, cols, value):
        at = 0
        for first, count in rows:
            if index is None:
                ref[pl.ds(first, count), cols] = value[at:at + count]
            else:
                ref[index, pl.ds(first, count), cols] = value[at:at + count]
            at += count

    def qk_body(i, carry):
        value = product(lambda k0, depth: w_qkv[i, k0:k0 + depth, :])
        put(qkv_out, i, slice(None), rotate(value, cos_of(), sin_of()))
        return carry

    lax.fori_loop(0, 2, qk_body, 0)
    put(qkv_out, 2, slice(None), product(lambda k0, depth: w_qkv[2, k0:k0 + depth, :]).astype(BF16))
    tile = min(256, w_in.shape[1])

    def in_body(n, carry):
        cols = pl.ds(pl.multiple_of(n * tile, tile), tile)
        pre = product(lambda k0, depth: w_in[k0:k0 + depth, cols]) + b_in_of(cols).astype(F32)
        put(act_out, None, cols, jax.nn.gelu(pre, approximate=True).astype(BF16))
        return carry

    lax.fori_loop(0, w_in.shape[1] // tile, in_body, 0)


def first_kernel(x_ref, cos_ref, sin_ref, gain_ref, bias_ref, wq_ref, wk_ref, wv_ref, w_in_ref, b_in_ref,
                 qkv_ref, act_ref, normed, w_qkv, w_in, sems):
    step = pl.program_id(0)
    copies = [pltpu.make_async_copy(w.at[0], w_qkv.at[i], sems.at[i]) for i, w in enumerate((wq_ref, wk_ref, wv_ref))]
    copies.append(pltpu.make_async_copy(w_in_ref.at[0], w_in, sems.at[3]))

    @pl.when(step == 0)
    def _():
        for copy in copies:
            copy.start()

    gain, bias = gain_ref[0:1].astype(F32), bias_ref[0:1].astype(F32)
    group = 16

    def body(g, carry):
        rows = pl.ds(pl.multiple_of(g * group, group), group)
        normed[rows, :] = norm_rows(x_ref[rows, :].astype(F32), gain, bias)
        return carry

    lax.fori_loop(0, x_ref.shape[0] // group, body, 0)

    @pl.when(step == 0)
    def _():
        for copy in copies:
            copy.wait()

    depth = normed.shape[1] // STREAMS
    project(lambda i: normed[:, i * depth:(i + 1) * depth], [(0, normed.shape[0])],
            lambda: cos_ref[...], lambda: sin_ref[...], w_qkv, w_in, lambda cols: b_in_ref[0:1, cols], qkv_ref, act_ref)


def first_projection(x, cos, sin, ln_gain, ln_bias, w_q, w_k, w_v, w_in, b_in):
    rows, width = x.shape
    head, ff = w_q.shape[2], w_in.shape[2]
    block = 256
    whole = lambda a: pl.BlockSpec(a.shape, lambda g: (0,) * a.ndim)
    any_spec = pl.BlockSpec(memory_space=pl.ANY)
    return pl.pallas_call(
        first_kernel,
        grid=(rows // block,),
        in_specs=[pl.BlockSpec((block, width), lambda g: (g, 0)), pl.BlockSpec((block, 128), lambda g: (g, 0)),
                  pl.BlockSpec((block, 128), lambda g: (g, 0)), whole(ln_gain), whole(ln_bias),
                  any_spec, any_spec, any_spec, any_spec, whole(b_in)],
        out_specs=[pl.BlockSpec((3, block, head), lambda g: (0, g, 0)), pl.BlockSpec((block, ff), lambda g: (g, 0))],
        out_shape=[jax.ShapeDtypeStruct((3, rows, head), BF16), jax.ShapeDtypeStruct((rows, ff), BF16)],
        scratch_shapes=[pltpu.VMEM((block, width), BF16), pltpu.VMEM((3, width, head), BF16),
                        pltpu.VMEM((width, ff), BF16), pltpu.SemaphoreType.DMA((4,))],
        compiler_params=pltpu.CompilerParams(vmem_limit_bytes=VMEM_LIMIT, dimension_semantics=("arbitrary",)),
        name="first_projection",
    )(x, cos, sin, ln_gain, ln_bias, w_q, w_k, w_v, w_in, b_in)


def attend_kernel(pos_row_ref, pos_lane_ref, qkv_ref, k_ref, v_ref, *rest):
    ctx_ref, k_out_ref, v_out_ref = rest[-3:]
    steps, batch, dim = qkv_ref.shape[1:]
    slots = k_ref.shape[1]
    flat = lambda i: qkv_ref[i].astype(F32).reshape(steps * batch, dim).astype(BF16)
    query, key, value = flat(0), flat(1), flat(2)
    n_rows, n_cols = steps * batch, batch * slots
    place_row = lax.broadcasted_iota(jnp.int32, (n_cols, n_rows), 0)
    place_col = lax.broadcasted_iota(jnp.int32, (n_cols, n_rows), 1)
    hit = (lax.div(place_row, slots) == lax.rem(place_col, batch)) & (lax.rem(place_row, slots) == pos_lane_ref[0])
    one_hot = jnp.where(hit, 1.0, 0.0)
    written = jnp.sum(one_hot, axis=1, keepdims=True) > 0.5
    one_hot = one_hot.astype(BF16)
    caches = []
    for new, old_ref, out_ref in ((key, k_ref, k_out_ref), (value, v_ref, v_out_ref)):
        placed = jnp.dot(one_hot, new, preferred_element_type=F32)
        cache = jnp.where(written, placed, old_ref[...].reshape(n_cols, dim).astype(F32)).astype(BF16)
        out_ref[...] = cache.reshape(batch, slots, dim)
        caches.append(cache)
    scores = lax.dot_general(query, caches[0], (((1,), (1,)), ((), ())), preferred_element_type=F32) * (dim ** -0.5)
    row = lax.broadcasted_iota(jnp.int32, (n_rows, n_cols), 0)
    col = lax.broadcasted_iota(jnp.int32, (n_rows, n_cols), 1)
    visible = (lax.rem(row, batch) == lax.div(col, slots)) & (lax.rem(col, slots) <= pos_row_ref[0])
    scores = jnp.where(visible, scores, -jnp.inf)
    exp_scores = jnp.exp(scores - jnp.max(scores, axis=-1, keepdims=True))
    probs = (exp_scores / jnp.sum(exp_scores, axis=-1, keepdims=True)).astype(BF16)
    context = jnp.dot(probs, caches[1], preferred_element_type=F32)
    ctx_ref[...] = context.reshape(steps, batch, dim).astype(BF16)


def attention(layer, pos_row, pos_lane, qkv, k_cache, v_cache, carried):
    n_layers, batch, slots, dim = k_cache.shape
    steps = qkv.shape[1] // batch
    block = pos_row.shape[1] // steps
    cache_spec = pl.BlockSpec((None, block, slots, dim), lambda g: (layer, g, 0, 0))
    extra = list(carried)
    ctx, k_out, v_out = pl.pallas_call(
        attend_kernel,
        grid=(batch // block,),
        in_specs=[pl.BlockSpec((1,) + pos_row.shape[1:], lambda g: (g, 0, 0)),
                  pl.BlockSpec((1,) + pos_lane.shape[1:], lambda g: (g, 0, 0)),
                  pl.BlockSpec((3, steps, block, dim), lambda g: (0, 0, g, 0)), cache_spec, cache_spec]
        + [pl.BlockSpec(memory_space=pl.ANY)] * len(extra),
        out_specs=[pl.BlockSpec((steps, block, dim), lambda g: (0, g, 0)), cache_spec, cache_spec],
        out_shape=[jax.ShapeDtypeStruct((steps, batch, dim), BF16)] + [jax.ShapeDtypeStruct(k_cache.shape, BF16)] * 2,
        input_output_aliases={5: 1, 6: 2} if extra else {},
        compiler_params=pltpu.CompilerParams(vmem_limit_bytes=VMEM_LIMIT, dimension_semantics=("arbitrary",)),
        name=f"attention_{layer}",
    )(pos_row, pos_lane, qkv.reshape(3, steps, batch, dim), k_cache, v_cache, *extra)
    return ctx.reshape(steps * batch, dim), (k_out, v_out)


def sum_kernel(layer, last, *refs):
    if last:
        (ctx_ref, act_ref, hid_ref, b_out_ref, w_o_ref, w_out_ref,
         out_ref,
         w_cat, lhs, pbuf, sib_in, ring_in, full, hid, local_sem,
         sib_s, sib_r, ring_s, ring_r, ag_s, ag_r, agsib_s, agsib_r, put_sem) = refs
    else:
        (ctx_ref, act_ref, x_ref, b_out_ref, w_o_ref, w_out_ref,
         gain_ref, bias_ref, cos_ref, sin_ref, b_in_ref, wq_ref, wk_ref, wv_ref, w_in_ref,
         qkv_ref, act_out_ref, hid_ref,
         w_cat, lhs, pbuf, sib_in, ring_in, full, hid, local_sem,
         sib_s, sib_r, ring_s, ring_r, ag_s, ag_r, agsib_s, agsib_r,
         w_qkv, w_in, w_sem) = refs
    me = lax.axis_index("tp")
    chip, core = lax.div(me, 2), lax.rem(me, 2)
    pos = ring_of_chip(chip)
    right = {"tp": 2 * chip_of_ring(pos + 1) + core}
    left = {"tp": 2 * chip_of_ring(pos - 1) + core}
    sibling = {"tp": 2 * chip + 1 - core}
    chip_at = {off: chip_of_ring(pos + off) for off in OFFSETS}
    toward = (right, left)
    batch, part = pbuf.shape[3], pbuf.shape[4]
    pair = 2 * batch
    d_ctx = ctx_ref.shape[1]

    loads = []
    for i in range(STREAMS):
        cols = slice(i * part, (i + 1) * part)
        loads.append((pltpu.make_async_copy(w_o_ref.at[layer, :, cols], w_cat.at[i, 0:d_ctx, :], local_sem.at[2 * i]),
                      pltpu.make_async_copy(w_out_ref.at[layer, :, cols], w_cat.at[i, d_ctx:, :], local_sem.at[2 * i + 1])))
    for both in loads:
        for copy in both:
            copy.start()
    if last:
        own_load = pltpu.make_async_copy(hid_ref, hid, local_sem.at[2 * STREAMS])
    else:
        own_load = pltpu.make_async_copy(x_ref.at[me], hid, local_sem.at[2 * STREAMS])
        w_loads = [pltpu.make_async_copy(w.at[layer + 1], w_qkv.at[i], w_sem.at[i]) for i, w in enumerate((wq_ref, wk_ref, wv_ref))]
        w_loads.append(pltpu.make_async_copy(w_in_ref.at[layer + 1], w_in, w_sem.at[3]))
    own_load.start()

    barrier = pltpu.get_barrier_semaphore()
    for peer in (left, right, sibling):
        pl.semaphore_signal(barrier, inc=1, device_id=peer, device_id_type=pl.DeviceIdType.MESH)
    pl.semaphore_wait(barrier, 3)

    def remote(src, dst, send_sem, recv_sem, device):
        return pltpu.make_async_remote_copy(src_ref=src, dst_ref=dst, send_sem=send_sem, recv_sem=recv_sem,
                                            device_id=device, device_id_type=pl.DeviceIdType.MESH)

    def sib_copy(slot, i):
        return remote(pbuf.at[slot, i, 1 - core], sib_in.at[slot, i], sib_s.at[slot, i], sib_r.at[slot, i], sibling)

    def ring_copy(way, hop, i):
        slot = SLOT[4 - hop] if way == 0 else SLOT[hop - 4]
        return remote(pbuf.at[slot, i, core], ring_in.at[way, hop, i], ring_s.at[way, hop, i], ring_r.at[way, hop, i], toward[way])

    def gather_copy(way, hop, i):
        sign = -1 if way == 0 else 1
        src, dst = SLOT[sign * (hop - 1)], SLOT[sign * hop]
        return remote(full.at[i, src, core], full.at[i, dst, core], ag_s.at[way, hop - 1, i], ag_r.at[way, hop - 1, i], toward[way])

    def gather_sib(slot, i):
        return remote(full.at[i, slot, core], full.at[i, slot, core], agsib_s.at[slot, i], agsib_r.at[slot, i], sibling)

    def partials(offs):
        for j, off in enumerate(offs):
            rows = pl.ds(pl.multiple_of(chip_at[off] * pair, pair), pair)
            lhs[j * pair:(j + 1) * pair, :d_ctx] = ctx_ref[rows, :]
            lhs[j * pair:(j + 1) * pair, d_ctx:] = act_ref[rows, :]
        count = len(offs) * pair
        tile = min(256, part)
        for i in range(STREAMS):
            if offs[0] == 4:
                for copy in loads[i]:
                    copy.wait()

            def body(n, carry, i=i):
                cols = pl.ds(pl.multiple_of(n * tile, tile), tile)
                value = jnp.dot(lhs[:count, :], w_cat[i, :, cols], preferred_element_type=F32).astype(BF16)
                for j, off in enumerate(offs):
                    for c in range(2):
                        at = j * pair + c * batch
                        pbuf[SLOT[off], i, c, :, cols] = value[at:at + batch]
                return carry

            lax.fori_loop(0, part // tile, body, 0)
            for off in offs:
                sib_copy(SLOT[off], i).start()

    def add_up(slot, i, ring_terms):
        total = pbuf[slot, i, core].astype(F32) + sib_in[slot, i].astype(F32)
        for term in ring_terms:
            total = total + term.astype(F32)
        return total

    def has_fourth(way, i):
        return (i < STREAMS // 2) == (way == 0)

    partials([4])
    if not last:
        for copy in w_loads:
            copy.start()
    for i in range(STREAMS):
        sib_copy(7, i).wait_recv()
        pbuf[7, i, core] = add_up(7, i, []).astype(BF16)
        ring_copy(0 if has_fourth(0, i) else 1, 0, i).start()
    for hop in range(1, 4):
        partials([hop - 4, 4 - hop])
        order = (2, 3, 0, 1) if hop == 1 else (0, 1, 2, 3)
        for i in order:
            for way in range(2):
                k = i if way == 0 else STREAMS - 1 - i
                slot = SLOT[4 - hop] if way == 0 else SLOT[hop - 4]
                sib_copy(slot, k).wait_recv()
                terms = []
                if hop > 1 or has_fourth(way, k):
                    ring_copy(way, hop - 1, k).wait_recv()
                    terms.append(ring_in[way, hop - 1, k])
                pbuf[slot, k, core] = add_up(slot, k, terms).astype(BF16)
                ring_copy(way, hop, k).start()
    partials([0])
    own_load.wait()
    for i in range(STREAMS):
        cols = slice(i * part, (i + 1) * part)
        sib_copy(0, i).wait_recv()
        terms = []
        for way in range(2):
            ring_copy(way, 3, i).wait_recv()
            terms.append(ring_in[way, 3, i])
        total = hid[:, cols].astype(F32) + add_up(0, i, terms) + b_out_ref[layer:layer + 1, cols].astype(F32)
        hid[:, cols] = total.astype(BF16)
        if last:
            full[i, 0, core] = total.astype(BF16)
            for way in range(2):
                gather_copy(way, 1, i).start()
            gather_sib(0, i).start()
    if not last:
        gain, bias = gain_ref[layer + 1:layer + 2].astype(F32), bias_ref[layer + 1:layer + 2].astype(F32)
        group = 16

        def norm_body(g, carry):
            rows = pl.ds(pl.multiple_of(g * group, group), group)
            normed = norm_rows(hid[rows, :].astype(F32), gain, bias)
            for i in range(STREAMS):
                full[i, 0, core, rows, :] = normed[:, i * part:(i + 1) * part]
            return carry

        lax.fori_loop(0, batch // group, norm_body, 0)
        for i in range(STREAMS):
            for way in range(2):
                gather_copy(way, 1, i).start()
            gather_sib(0, i).start()
        hid_ref[...] = hid[...]
        for copy in w_loads:
            copy.wait()

    def use(offs):
        for off in offs:
            for i in range(STREAMS):
                gather_sib(SLOT[off], i).wait_recv()
        if last:
            for off in offs:
                for i in range(STREAMS):
                    put(off, i).start()
            return
        first, count = SLOT[offs[0]], len(offs)

        def table(ref):
            return jnp.concatenate([ref[pl.ds(pl.multiple_of(chip_at[off] * pair, pair), pair), :] for off in offs], axis=0)

        project(lambda i: full[i, first:first + count].reshape(count * pair, part),
                [(pl.multiple_of(chip_at[off] * pair, pair), pair) for off in offs],
                lambda: table(cos_ref), lambda: table(sin_ref), w_qkv, w_in, lambda cols: b_in_ref[layer + 1:layer + 2, cols],
                qkv_ref, act_out_ref)

    def put(off, i):
        slot = SLOT[off]
        return pltpu.make_async_copy(full.at[i, slot], out_ref.at[pl.ds(2 * chip_at[off], 2), :, i * part:(i + 1) * part], put_sem.at[slot, i])

    use([0])
    for hop in range(2, 5):
        for i in range(STREAMS):
            for way in range(2):
                k = i if way == 0 else STREAMS - 1 - i
                gather_copy(way, hop - 1, k).wait_recv()
                if hop < 4 or has_fourth(way, k):
                    gather_copy(way, hop, k).start()
                gather_sib(SLOT[1 - hop] if way == 0 else SLOT[hop - 1], k).start()
        use([1 - hop, hop - 1])
    for i in range(STREAMS):
        gather_copy(0 if has_fourth(0, i) else 1, 4, i).wait_recv()
        gather_sib(7, i).start()
    use([4])

    for i in range(STREAMS):
        for slot in range(CHIPS):
            sib_copy(slot, i).wait_send()
            gather_sib(slot, i).wait_send()
        for way in range(2):
            for hop in range(4):
                if hop > 0 or has_fourth(way, i):
                    ring_copy(way, hop, i).wait_send()
                if hop < 3 or has_fourth(way, i):
                    gather_copy(way, hop + 1, i).wait_send()
        if last:
            for off in OFFSETS:
                put(off, i).wait()


def sum_over_tp(layer, ctx, act, own, b_out, w_o, w_out, rest=None):
    rows, d_ctx = ctx.shape
    ff, width = act.shape[1], w_o.shape[2]
    batch, part = rows // TP, width // STREAMS
    last = rest is None
    vmem, hbm = pl.BlockSpec(memory_space=pltpu.VMEM), pl.BlockSpec(memory_space=pl.ANY)
    dma = pltpu.SemaphoreType.DMA
    scratch = [pltpu.VMEM((STREAMS, d_ctx + ff, part), BF16), pltpu.VMEM((4 * batch, d_ctx + ff), BF16),
               pltpu.VMEM((CHIPS, STREAMS, 2, batch, part), BF16), pltpu.VMEM((CHIPS, STREAMS, batch, part), BF16),
               pltpu.VMEM((2, 4, STREAMS, batch, part), BF16), pltpu.VMEM((STREAMS, CHIPS, 2, batch, part), BF16),
               pltpu.VMEM((batch, width), BF16), dma((2 * STREAMS + 1,)),
               dma((CHIPS, STREAMS)), dma((CHIPS, STREAMS)), dma((2, 4, STREAMS)), dma((2, 4, STREAMS)),
               dma((2, 4, STREAMS)), dma((2, 4, STREAMS)), dma((CHIPS, STREAMS)), dma((CHIPS, STREAMS))]
    params = pltpu.CompilerParams(collective_id=layer, has_side_effects=True, vmem_limit_bytes=VMEM_LIMIT)
    if last:
        return pl.pallas_call(
            functools.partial(sum_kernel, layer, True),
            in_specs=[vmem, vmem, hbm, vmem, hbm, hbm],
            out_specs=hbm,
            out_shape=jax.ShapeDtypeStruct((TP, batch, width), BF16),
            scratch_shapes=scratch + [dma((CHIPS, STREAMS))],
            compiler_params=params, name=f"sum_{layer}",
        )(ctx, act, own, b_out, w_o, w_out)
    gain, bias, cos, sin, b_in, w_q, w_k, w_v, w_in = rest
    return pl.pallas_call(
        functools.partial(sum_kernel, layer, False),
        in_specs=[vmem, vmem, hbm, vmem, hbm, hbm, vmem, vmem, vmem, vmem, vmem, hbm, hbm, hbm, hbm],
        out_specs=[vmem, vmem, vmem],
        out_shape=[jax.ShapeDtypeStruct((3, rows, d_ctx), BF16), jax.ShapeDtypeStruct((rows, ff), BF16),
                   jax.ShapeDtypeStruct((batch, width), BF16)],
        scratch_shapes=scratch + [pltpu.VMEM((3, width, d_ctx), BF16), pltpu.VMEM((width, ff), BF16), dma((4,))],
        compiler_params=params, name=f"sum_{layer}",
    )(ctx, act, own, b_out, w_o, w_out, gain, bias, cos, sin, b_in, w_q, w_k, w_v, w_in)


def rotary_tables(positions):
    inv_freq = 1.0 / (10000.0 ** (jnp.arange(0, ROT_DIM, 2).astype(F32) / ROT_DIM))
    angles = positions.astype(F32)[:, None] * inv_freq[None, :]
    cos = jnp.repeat(jnp.cos(angles), 2, axis=1)
    sin = jnp.repeat(jnp.sin(angles), 2, axis=1) * jnp.where(jnp.arange(ROT_DIM) % 2 == 0, -1.0, 1.0)
    rest = 128 - ROT_DIM
    return jnp.pad(cos, ((0, 0), (0, rest)), constant_values=1.0), jnp.pad(sin, ((0, 0), (0, rest)))


def decode_shard(x_steps, cur_len, k_cache, v_cache, ln_gain, ln_bias, w_q, w_k, w_v, w_o, w_in, b_in, w_out, b_out):
    n_layers, batch, slots, _, dim = k_cache.shape
    steps, _, width = x_steps.shape
    rows = steps * batch
    pos = cur_len[None, :] + jnp.arange(steps, dtype=jnp.int32)[:, None]
    cos, sin = rotary_tables(pos.reshape(rows))
    block = 8
    grouped = pos.reshape(steps, batch // block, block).transpose(1, 0, 2).reshape(batch // block, steps * block)
    pos_row, pos_lane = grouped[:, :, None], grouped[:, None, :]
    k_old, v_old = k_cache.reshape(n_layers, batch, slots, dim), v_cache.reshape(n_layers, batch, slots, dim)

    qkv, act = first_projection(x_steps.reshape(rows, width), cos, sin, ln_gain, ln_bias, w_q, w_k, w_v, w_in, b_in)
    ctx, caches = attention(0, pos_row, pos_lane, qkv, k_old, v_old, ())
    qkv, act, own = sum_over_tp(0, ctx, act, x_steps, b_out, w_o, w_out,
                                (ln_gain, ln_bias, cos, sin, b_in, w_q, w_k, w_v, w_in))
    ctx, caches = attention(1, pos_row, pos_lane, qkv, k_old, v_old, caches)
    hidden = sum_over_tp(1, ctx, act, own, b_out, w_o, w_out)
    return hidden, caches[0].reshape(k_cache.shape), caches[1].reshape(v_cache.shape)


def solution(mesh):
    cache_spec = P(None, "dp", None, "tp", None)
    in_specs = (P(None, "dp", None), P("dp"), cache_spec, cache_spec, P(None, None), P(None, None),
                P(None, None, "tp"), P(None, None, "tp"), P(None, None, "tp"), P(None, "tp", None),
                P(None, None, "tp"), P(None, "tp"), P(None, "tp", None), P(None, None))
    out_specs = (P(None, "dp", None), cache_spec, cache_spec)
    return jax.shard_map(decode_shard, mesh=mesh, in_specs=in_specs, out_specs=out_specs, check_vma=False)
```

```python
import functools

import jax
import jax.numpy as jnp
import numpy as np
from jax import lax
from jax.experimental import pallas as pl
from jax.experimental.pallas import tpu as pltpu
from jax.sharding import PartitionSpec as P

ROT_DIM = 64
LN_EPS = 1e-5
TP = 16
CHIPS = 8
STREAMS = 4
BF16 = jnp.bfloat16
F32 = jnp.float32
VMEM_LIMIT = 67_000_000
SLOT = {0: 0, -1: 1, 1: 2, -2: 3, 2: 4, -3: 5, 3: 6, 4: 7, -4: 7}
OFFSETS = (0, -1, 1, -2, 2, -3, 3, 4)


def ring_of_chip(chip):
    z, y = lax.div(chip, 2), lax.rem(chip, 2)
    return z + y * (7 - 2 * z)


def chip_of_ring(pos):
    pos = lax.rem(pos + 2 * CHIPS, CHIPS)
    y = lax.div(pos, 4)
    z = pos + y * (7 - 2 * pos)
    return 2 * z + y


def norm_rows(load, store, gain_ref, bias_ref, layer, width):
    starts = range(0, width, 128)
    total = load(0).astype(F32)
    for col in starts[1:]:
        total = total + load(col).astype(F32)
    mean = jnp.sum(total, axis=-1, keepdims=True) * (1.0 / width)
    square = jnp.zeros_like(total)
    for col in starts:
        centered = load(col).astype(F32) - mean
        square = square + centered * centered
    scale = lax.rsqrt(jnp.sum(square, axis=-1, keepdims=True) * (1.0 / width) + LN_EPS)
    for col in starts:
        gain = gain_ref[layer:layer + 1, col:col + 128].astype(F32)
        bias = bias_ref[layer:layer + 1, col:col + 128].astype(F32)
        store(col, ((load(col).astype(F32) - mean) * scale * gain + bias).astype(BF16))


def rotate(vec, cos, sin):
    head, rest = vec[:, :128], vec[:, 128:]
    even = lax.rem(lax.broadcasted_iota(jnp.int32, head.shape, 1), 2) == 0
    swapped = jnp.where(even, pltpu.roll(head, 127, 1), pltpu.roll(head, 1, 1))
    return jnp.concatenate([head * cos + swapped * sin, rest], axis=1).astype(BF16)


def project(lhs_piece, rows, cos_of, sin_of, w_qkv, w_in, b_in_of, qkv_out, act_out):
    def product(w_ref_cols):
        total = None
        for i in range(STREAMS):
            lhs = lhs_piece(i)
            depth = lhs.shape[1]
            term = jnp.dot(lhs, w_ref_cols(i * depth, depth), preferred_element_type=F32)
            total = term if total is None else total + term
        return total

    def put(ref, index, cols, value):
        at = 0
        for first, count in rows:
            if index is None:
                ref[pl.ds(first, count), cols] = value[at:at + count]
            else:
                ref[index, pl.ds(first, count), cols] = value[at:at + count]
            at += count

    def qk_body(i, carry):
        value = product(lambda k0, depth: w_qkv[i, k0:k0 + depth, :])
        put(qkv_out, i, slice(None), rotate(value, cos_of(), sin_of()))
        return carry

    lax.fori_loop(0, 2, qk_body, 0)
    put(qkv_out, 2, slice(None), product(lambda k0, depth: w_qkv[2, k0:k0 + depth, :]).astype(BF16))
    tile = min(512, w_in.shape[1])

    def in_body(n, carry):
        cols = pl.ds(pl.multiple_of(n * tile, tile), tile)
        pre = product(lambda k0, depth: w_in[k0:k0 + depth, cols]) + b_in_of(cols).astype(F32)
        put(act_out, None, cols, jax.nn.gelu(pre, approximate=True).astype(BF16))
        return carry

    lax.fori_loop(0, w_in.shape[1] // tile, in_body, 0)


def first_kernel(x_ref, cos_ref, sin_ref, gain_ref, bias_ref, wq_ref, wk_ref, wv_ref, w_in_ref, b_in_ref,
                 qkv_ref, act_ref, normed, w_qkv, w_in, sems):
    step = pl.program_id(0)
    copies = [pltpu.make_async_copy(w.at[0], w_qkv.at[i], sems.at[i]) for i, w in enumerate((wq_ref, wk_ref, wv_ref))]
    copies.append(pltpu.make_async_copy(w_in_ref.at[0], w_in, sems.at[3]))

    @pl.when(step == 0)
    def _():
        for copy in copies:
            copy.start()

    group = 64

    def body(g, carry):
        rows = pl.ds(pl.multiple_of(g * group, group), group)

        def store(col, value):
            normed[rows, col:col + 128] = value

        norm_rows(lambda col: x_ref[rows, col:col + 128], store, gain_ref, bias_ref, 0, normed.shape[1])
        return carry

    lax.fori_loop(0, x_ref.shape[0] // group, body, 0)

    @pl.when(step == 0)
    def _():
        for copy in copies:
            copy.wait()

    depth = normed.shape[1] // STREAMS
    project(lambda i: normed[:, i * depth:(i + 1) * depth], [(0, normed.shape[0])],
            lambda: cos_ref[...], lambda: sin_ref[...], w_qkv, w_in, lambda cols: b_in_ref[0:1, cols], qkv_ref, act_ref)


def first_projection(x, cos, sin, ln_gain, ln_bias, w_q, w_k, w_v, w_in, b_in):
    rows, width = x.shape
    head, ff = w_q.shape[2], w_in.shape[2]
    block = 512 if rows % 512 == 0 else 256
    whole = lambda a: pl.BlockSpec(a.shape, lambda g: (0,) * a.ndim)
    any_spec = pl.BlockSpec(memory_space=pl.ANY)
    return pl.pallas_call(
        first_kernel,
        grid=(rows // block,),
        in_specs=[pl.BlockSpec((block, width), lambda g: (g, 0)), pl.BlockSpec((block, 128), lambda g: (g, 0)),
                  pl.BlockSpec((block, 128), lambda g: (g, 0)), whole(ln_gain), whole(ln_bias),
                  any_spec, any_spec, any_spec, any_spec, whole(b_in)],
        out_specs=[pl.BlockSpec((3, block, head), lambda g: (0, g, 0)), pl.BlockSpec((block, ff), lambda g: (g, 0))],
        out_shape=[jax.ShapeDtypeStruct((3, rows, head), BF16), jax.ShapeDtypeStruct((rows, ff), BF16)],
        scratch_shapes=[pltpu.VMEM((block, width), BF16), pltpu.VMEM((3, width, head), BF16),
                        pltpu.VMEM((width, ff), BF16), pltpu.SemaphoreType.DMA((4,))],
        compiler_params=pltpu.CompilerParams(vmem_limit_bytes=VMEM_LIMIT, dimension_semantics=("arbitrary",)),
        name="first_projection",
    )(x, cos, sin, ln_gain, ln_bias, w_q, w_k, w_v, w_in, b_in)


def attend_kernel(pos_row_ref, pos_lane_ref, qkv_ref, k_ref, v_ref, *rest):
    ctx_ref, k_out_ref, v_out_ref = rest[-3:]
    steps, batch, dim = qkv_ref.shape[1:]
    slots = k_ref.shape[1]
    flat = lambda i: qkv_ref[i].astype(F32).reshape(steps * batch, dim).astype(BF16)
    query, key, value = flat(0), flat(1), flat(2)
    n_rows, n_cols = steps * batch, batch * slots
    place_row = lax.broadcasted_iota(jnp.int32, (n_cols, n_rows), 0)
    place_col = lax.broadcasted_iota(jnp.int32, (n_cols, n_rows), 1)
    log = slots.bit_length() - 1
    hit = ((place_row >> log) == (place_col & (batch - 1))) & ((place_row & (slots - 1)) == pos_lane_ref[0])
    one_hot = jnp.where(hit, 1.0, 0.0)
    written = jnp.sum(one_hot, axis=1, keepdims=True) > 0.5
    one_hot = one_hot.astype(BF16)
    caches = []
    for new, old_ref, out_ref in ((key, k_ref, k_out_ref), (value, v_ref, v_out_ref)):
        placed = jnp.dot(one_hot, new, preferred_element_type=F32)
        cache = jnp.where(written, placed, old_ref[...].reshape(n_cols, dim).astype(F32)).astype(BF16)
        out_ref[...] = cache.reshape(batch, slots, dim)
        caches.append(cache)
    scores = lax.dot_general(query, caches[0], (((1,), (1,)), ((), ())), preferred_element_type=F32) * (dim ** -0.5)
    row = lax.broadcasted_iota(jnp.int32, (n_rows, n_cols), 0)
    col = lax.broadcasted_iota(jnp.int32, (n_rows, n_cols), 1)
    visible = ((row & (batch - 1)) == (col >> log)) & ((col & (slots - 1)) <= pos_row_ref[0])
    scores = jnp.where(visible, scores, -jnp.inf)
    exp_scores = jnp.exp(scores - jnp.max(scores, axis=-1, keepdims=True))
    probs = (exp_scores / jnp.sum(exp_scores, axis=-1, keepdims=True)).astype(BF16)
    context = jnp.dot(probs, caches[1], preferred_element_type=F32)
    ctx_ref[...] = context.reshape(steps, batch, dim).astype(BF16)


def attention(layer, pos_row, pos_lane, qkv, k_cache, v_cache, carried):
    n_layers, batch, slots, dim = k_cache.shape
    steps = qkv.shape[1] // batch
    block = pos_row.shape[1] // steps
    cache_spec = pl.BlockSpec((None, block, slots, dim), lambda g: (layer, g, 0, 0))
    extra = list(carried)
    ctx, k_out, v_out = pl.pallas_call(
        attend_kernel,
        grid=(batch // block,),
        in_specs=[pl.BlockSpec((1,) + pos_row.shape[1:], lambda g: (g, 0, 0)),
                  pl.BlockSpec((1,) + pos_lane.shape[1:], lambda g: (g, 0, 0)),
                  pl.BlockSpec((3, steps, block, dim), lambda g: (0, 0, g, 0)), cache_spec, cache_spec]
        + [pl.BlockSpec(memory_space=pl.ANY)] * len(extra),
        out_specs=[pl.BlockSpec((steps, block, dim), lambda g: (0, g, 0)), cache_spec, cache_spec],
        out_shape=[jax.ShapeDtypeStruct((steps, batch, dim), BF16)] + [jax.ShapeDtypeStruct(k_cache.shape, BF16)] * 2,
        input_output_aliases={5: 1, 6: 2} if extra else {},
        compiler_params=pltpu.CompilerParams(vmem_limit_bytes=VMEM_LIMIT, dimension_semantics=("arbitrary",)),
        name=f"attention_{layer}",
    )(pos_row, pos_lane, qkv.reshape(3, steps, batch, dim), k_cache, v_cache, *extra)
    return ctx.reshape(steps * batch, dim), (k_out, v_out)


def sum_kernel(layer, last, *refs):
    if last:
        (ctx_ref, act_ref, hid_ref, b_out_ref, w_o_ref, w_out_ref,
         out_ref,
         w_cat, lhs, pbuf, sib_in, ring_in, hid, local_sem,
         sib_s, sib_r, ring_s, ring_r, ag_s, ag_r, agsib_s, agsib_r) = refs
    else:
        (ctx_ref, act_ref, x_ref, b_out_ref, w_o_ref, w_out_ref,
         gain_ref, bias_ref, cos_ref, sin_ref, b_in_ref, wq_ref, wk_ref, wv_ref, w_in_ref,
         qkv_ref, act_out_ref, hid_ref,
         w_cat, lhs, pbuf, sib_in, ring_in, full, hid, local_sem,
         sib_s, sib_r, ring_s, ring_r, ag_s, ag_r, agsib_s, agsib_r,
         w_qkv, w_in, w_sem) = refs
    me = lax.axis_index("tp")
    chip, core = lax.div(me, 2), lax.rem(me, 2)
    pos = ring_of_chip(chip)
    right = {"tp": 2 * chip_of_ring(pos + 1) + core}
    left = {"tp": 2 * chip_of_ring(pos - 1) + core}
    sibling = {"tp": 2 * chip + 1 - core}
    chip_at = {off: chip_of_ring(pos + off) for off in OFFSETS}
    toward = (right, left)
    batch, part = pbuf.shape[3], pbuf.shape[4]
    pair = 2 * batch
    d_ctx = ctx_ref.shape[1]

    loads = []
    for i in range(STREAMS):
        cols = slice(i * part, (i + 1) * part)
        loads.append((pltpu.make_async_copy(w_o_ref.at[layer, :, cols], w_cat.at[i, 0:d_ctx, :], local_sem.at[2 * i]),
                      pltpu.make_async_copy(w_out_ref.at[layer, :, cols], w_cat.at[i, d_ctx:, :], local_sem.at[2 * i + 1])))
    for both in loads:
        for copy in both:
            copy.start()
    if last:
        own_load = pltpu.make_async_copy(hid_ref, hid, local_sem.at[2 * STREAMS])
    else:
        own_load = pltpu.make_async_copy(x_ref.at[me], hid, local_sem.at[2 * STREAMS])
        w_loads = [pltpu.make_async_copy(w.at[layer + 1], w_qkv.at[i], w_sem.at[i]) for i, w in enumerate((wq_ref, wk_ref, wv_ref))]
        w_loads.append(pltpu.make_async_copy(w_in_ref.at[layer + 1], w_in, w_sem.at[3]))
    own_load.start()

    barrier = pltpu.get_barrier_semaphore()
    for peer in (left, right, sibling):
        pl.semaphore_signal(barrier, inc=1, device_id=peer, device_id_type=pl.DeviceIdType.MESH)
    pl.semaphore_wait(barrier, 3)

    def remote(src, dst, send_sem, recv_sem, device):
        return pltpu.make_async_remote_copy(src_ref=src, dst_ref=dst, send_sem=send_sem, recv_sem=recv_sem,
                                            device_id=device, device_id_type=pl.DeviceIdType.MESH)

    def sib_copy(slot, i):
        return remote(pbuf.at[slot, i, 1 - core], sib_in.at[slot, i], sib_s.at[slot, i], sib_r.at[slot, i], sibling)

    def ring_copy(way, hop, i):
        slot = SLOT[4 - hop] if way == 0 else SLOT[hop - 4]
        return remote(pbuf.at[slot, i, core], ring_in.at[way, hop, i], ring_s.at[way, hop, i], ring_r.at[way, hop, i], toward[way])

    def landing(off, i):
        return out_ref.at[2 * chip_at[off] + core, :, i * part:(i + 1) * part] if last else full.at[i, SLOT[off], core]

    def gather_copy(way, hop, i):
        sign = -1 if way == 0 else 1
        src = landing(sign * (hop - 1), i)
        dst = src if last else landing(sign * hop, i)
        return remote(src, dst, ag_s.at[way, hop - 1, i], ag_r.at[way, hop - 1, i], toward[way])

    def gather_sib(slot, i):
        off = OFFSETS[slot]
        return remote(landing(off, i), landing(off, i), agsib_s.at[slot, i], agsib_r.at[slot, i], sibling)

    def partials(offs, then=None):
        for j, off in enumerate(offs):
            rows = pl.ds(pl.multiple_of(chip_at[off] * pair, pair), pair)
            lhs[j * pair:(j + 1) * pair, :d_ctx] = ctx_ref[rows, :]
            lhs[j * pair:(j + 1) * pair, d_ctx:] = act_ref[rows, :]
        count = len(offs) * pair
        tile = min(512, part)
        for i in range(STREAMS):
            if offs[0] == 4:
                for copy in loads[i]:
                    copy.wait()

            def body(n, carry, i=i):
                cols = pl.ds(pl.multiple_of(n * tile, tile), tile)
                value = jnp.dot(lhs[:count, :], w_cat[i, :, cols], preferred_element_type=F32).astype(BF16)
                for j, off in enumerate(offs):
                    for c in range(2):
                        at = j * pair + c * batch
                        pbuf[SLOT[off], i, c, :, cols] = value[at:at + batch]
                return carry

            lax.fori_loop(0, part // tile, body, 0)
            for off in offs:
                sib_copy(SLOT[off], i).start()
            if then is not None and i > 0:
                then(i - 1)
        if then is not None:
            then(STREAMS - 1)

    def add_up(slot, i, ring_terms):
        total = pbuf[slot, i, core].astype(F32) + sib_in[slot, i].astype(F32)
        for term in ring_terms:
            total = total + term.astype(F32)
        return total

    def has_fourth(way, i):
        return (i < STREAMS // 2) == (way == 0)

    def start_ring(i):
        sib_copy(7, i).wait_recv()
        pbuf[7, i, core] = add_up(7, i, []).astype(BF16)
        ring_copy(0 if has_fourth(0, i) else 1, 0, i).start()

    def pass_on(hop, i):
        for way in range(2):
            k = i if way == 0 else STREAMS - 1 - i
            slot = SLOT[4 - hop] if way == 0 else SLOT[hop - 4]
            sib_copy(slot, k).wait_recv()
            terms = []
            if hop > 1 or has_fourth(way, k):
                ring_copy(way, hop - 1, k).wait_recv()
                terms.append(ring_in[way, hop - 1, k])
            pbuf[slot, k, core] = add_up(slot, k, terms).astype(BF16)
            ring_copy(way, hop, k).start()

    partials([4], start_ring)
    if not last:
        for copy in w_loads:
            copy.start()
    for hop in range(1, 4):
        partials([hop - 4, 4 - hop])
        for i in (2, 3, 0, 1) if hop == 1 else (0, 1, 2, 3):
            pass_on(hop, i)
    partials([0])
    own_load.wait()
    for i in range(STREAMS):
        cols = slice(i * part, (i + 1) * part)
        sib_copy(0, i).wait_recv()
        terms = []
        for way in range(2):
            ring_copy(way, 3, i).wait_recv()
            terms.append(ring_in[way, 3, i])
        total = hid[:, cols].astype(F32) + add_up(0, i, terms) + b_out_ref[layer:layer + 1, cols].astype(F32)
        if not last:
            hid[:, cols] = total.astype(BF16)
        if last:
            out_ref[me, :, cols] = total.astype(BF16)
            for way in range(2):
                gather_copy(way, 1, i).start()
            gather_sib(0, i).start()
    if not last:
        def store(col, value):
            at = col % part
            full[col // part, 0, core, :, at:at + 128] = value

        norm_rows(lambda col: hid[:, col:col + 128], store, gain_ref, bias_ref, layer + 1, STREAMS * part)
        for i in range(STREAMS):
            for way in range(2):
                gather_copy(way, 1, i).start()
            gather_sib(0, i).start()
        hid_ref[...] = hid[...]
        for copy in w_loads:
            copy.wait()

    def use(offs):
        for off in offs:
            for i in range(STREAMS):
                gather_sib(SLOT[off], i).wait_recv()
        if last:
            return
        first, count = SLOT[offs[0]], len(offs)

        def table(ref):
            return jnp.concatenate([ref[pl.ds(pl.multiple_of(chip_at[off] * pair, pair), pair), :] for off in offs], axis=0)

        project(lambda i: full[i, first:first + count].reshape(count * pair, part),
                [(pl.multiple_of(chip_at[off] * pair, pair), pair) for off in offs],
                lambda: table(cos_ref), lambda: table(sin_ref), w_qkv, w_in, lambda cols: b_in_ref[layer + 1:layer + 2, cols],
                qkv_ref, act_out_ref)

    use([0])
    for hop in range(2, 5):
        for i in range(STREAMS):
            for way in range(2):
                k = i if way == 0 else STREAMS - 1 - i
                gather_copy(way, hop - 1, k).wait_recv()
                if hop < 4 or has_fourth(way, k):
                    gather_copy(way, hop, k).start()
                gather_sib(SLOT[1 - hop] if way == 0 else SLOT[hop - 1], k).start()
        use([1 - hop, hop - 1])
    for i in range(STREAMS):
        gather_copy(0 if has_fourth(0, i) else 1, 4, i).wait_recv()
        gather_sib(7, i).start()
    use([4])

    for i in range(STREAMS):
        for slot in range(CHIPS):
            sib_copy(slot, i).wait_send()
            gather_sib(slot, i).wait_send()
        for way in range(2):
            for hop in range(4):
                if hop > 0 or has_fourth(way, i):
                    ring_copy(way, hop, i).wait_send()
                if hop < 3 or has_fourth(way, i):
                    gather_copy(way, hop + 1, i).wait_send()


def sum_over_tp(layer, ctx, act, own, b_out, w_o, w_out, rest=None):
    rows, d_ctx = ctx.shape
    ff, width = act.shape[1], w_o.shape[2]
    batch, part = rows // TP, width // STREAMS
    last = rest is None
    vmem, hbm = pl.BlockSpec(memory_space=pltpu.VMEM), pl.BlockSpec(memory_space=pl.ANY)
    dma = pltpu.SemaphoreType.DMA
    scratch = [pltpu.VMEM((STREAMS, d_ctx + ff, part), BF16), pltpu.VMEM((4 * batch, d_ctx + ff), BF16),
               pltpu.VMEM((CHIPS, STREAMS, 2, batch, part), BF16), pltpu.VMEM((CHIPS, STREAMS, batch, part), BF16),
               pltpu.VMEM((2, 4, STREAMS, batch, part), BF16)]
    if not last:
        scratch.append(pltpu.VMEM((STREAMS, CHIPS, 2, batch, part), BF16))
    scratch += [
               pltpu.VMEM((batch, width), BF16), dma((2 * STREAMS + 1,)),
               dma((CHIPS, STREAMS)), dma((CHIPS, STREAMS)), dma((2, 4, STREAMS)), dma((2, 4, STREAMS)),
               dma((2, 4, STREAMS)), dma((2, 4, STREAMS)), dma((CHIPS, STREAMS)), dma((CHIPS, STREAMS))]
    params = pltpu.CompilerParams(collective_id=layer, has_side_effects=True,
                                  vmem_limit_bytes=VMEM_LIMIT - 2 * TP * batch * width if last else VMEM_LIMIT)
    if last:
        return pl.pallas_call(
            functools.partial(sum_kernel, layer, True),
            in_specs=[vmem, vmem, hbm, vmem, hbm, hbm],
            out_specs=vmem,
            out_shape=pltpu.VMEM((TP, batch, width), BF16),
            scratch_shapes=scratch,
            compiler_params=params, name=f"sum_{layer}",
        )(ctx, act, own, b_out, w_o, w_out)
    gain, bias, cos, sin, b_in, w_q, w_k, w_v, w_in = rest
    return pl.pallas_call(
        functools.partial(sum_kernel, layer, False),
        in_specs=[vmem, vmem, hbm, vmem, hbm, hbm, vmem, vmem, vmem, vmem, vmem, hbm, hbm, hbm, hbm],
        out_specs=[vmem, vmem, vmem],
        out_shape=[jax.ShapeDtypeStruct((3, rows, d_ctx), BF16), jax.ShapeDtypeStruct((rows, ff), BF16),
                   jax.ShapeDtypeStruct((batch, width), BF16)],
        scratch_shapes=scratch + [pltpu.VMEM((3, width, d_ctx), BF16), pltpu.VMEM((width, ff), BF16), dma((4,))],
        compiler_params=params, name=f"sum_{layer}",
    )(ctx, act, own, b_out, w_o, w_out, gain, bias, cos, sin, b_in, w_q, w_k, w_v, w_in)


def rotary_tables(positions):
    lane = np.arange(128)
    exponent = (lane // 2 * 2).astype(np.float32) / ROT_DIM
    turned = lane < ROT_DIM
    inv_freq = jnp.where(turned, 1.0 / (10000.0 ** jnp.asarray(exponent, F32)), 0.0)
    sign = np.where(turned, np.where(lane % 2 == 0, -1.0, 1.0), 0.0).astype(np.float32)
    angles = positions.astype(F32)[:, None] * inv_freq[None, :]
    return jnp.cos(angles), jnp.sin(angles) * sign


def decode_shard(x_steps, cur_len, k_cache, v_cache, ln_gain, ln_bias, w_q, w_k, w_v, w_o, w_in, b_in, w_out, b_out):
    n_layers, batch, slots, _, dim = k_cache.shape
    steps, _, width = x_steps.shape
    rows = steps * batch
    pos = cur_len[None, :] + jnp.arange(steps, dtype=jnp.int32)[:, None]
    cos, sin = rotary_tables(pos.reshape(rows))
    block = 8
    grouped = pos.reshape(steps, batch // block, block).transpose(1, 0, 2).reshape(batch // block, steps * block)
    pos_row, pos_lane = grouped[:, :, None], grouped[:, None, :]
    k_old, v_old = k_cache.reshape(n_layers, batch, slots, dim), v_cache.reshape(n_layers, batch, slots, dim)

    qkv, act = first_projection(x_steps.reshape(rows, width), cos, sin, ln_gain, ln_bias, w_q, w_k, w_v, w_in, b_in)
    ctx, caches = attention(0, pos_row, pos_lane, qkv, k_old, v_old, ())
    qkv, act, own = sum_over_tp(0, ctx, act, x_steps, b_out, w_o, w_out,
                                (ln_gain, ln_bias, cos, sin, b_in, w_q, w_k, w_v, w_in))
    ctx, caches = attention(1, pos_row, pos_lane, qkv, k_old, v_old, caches)
    hidden = sum_over_tp(1, ctx, act, own, b_out, w_o, w_out)
    return hidden, caches[0].reshape(k_cache.shape), caches[1].reshape(v_cache.shape)


def solution(mesh):
    cache_spec = P(None, "dp", None, "tp", None)
    in_specs = (P(None, "dp", None), P("dp"), cache_spec, cache_spec, P(None, None), P(None, None),
                P(None, None, "tp"), P(None, None, "tp"), P(None, None, "tp"), P(None, "tp", None),
                P(None, None, "tp"), P(None, "tp"), P(None, "tp", None), P(None, None))
    out_specs = (P(None, "dp", None), cache_spec, cache_spec)
    return jax.shard_map(decode_shard, mesh=mesh, in_specs=in_specs, out_specs=out_specs, check_vma=False)
```

```python
import jax
import jax.numpy as jnp
from jax import lax
from jax.experimental import pallas as pl
from jax.experimental.pallas import tpu as pltpu
from jax.sharding import PartitionSpec as P

ROT_DIM = 64
LN_EPS = 1e-5
TP = 16
CHIPS = 8
STREAMS = 4
BF16 = jnp.bfloat16
F32 = jnp.float32
VMEM_LIMIT = 67_000_000
OFFSETS = (0, -1, 1, -2, 2, -3, 3, 4)
HALVES = 2
LAYERS = 2
GROUP = 8
SERVICE_US = 4.0


def ring_of_chip(chip):
    z, y = lax.div(chip, 2), lax.rem(chip, 2)
    return z + y * (7 - 2 * z)


def chip_of_ring(pos):
    pos = lax.rem(pos + 2 * CHIPS, CHIPS)
    y = lax.div(pos, 4)
    z = pos + y * (7 - 2 * pos)
    return 2 * z + y


def norm_rows(load, store, gain_ref, bias_ref, layer, width):
    starts = range(0, width, 128)
    total = load(0).astype(F32)
    for col in starts[1:]:
        total = total + load(col).astype(F32)
    mean = jnp.sum(total, axis=-1, keepdims=True) * (1.0 / width)
    square = jnp.zeros_like(total)
    for col in starts:
        centered = load(col).astype(F32) - mean
        square = square + centered * centered
    scale = lax.rsqrt(jnp.sum(square, axis=-1, keepdims=True) * (1.0 / width) + LN_EPS)
    for col in starts:
        gain = gain_ref[layer:layer + 1, col:col + 128].astype(F32)
        bias = bias_ref[layer:layer + 1, col:col + 128].astype(F32)
        store(col, ((load(col).astype(F32) - mean) * scale * gain + bias).astype(BF16))


def rotate(vec, cos, sin):
    head, rest = vec[:, :128], vec[:, 128:]
    even = lax.rem(lax.broadcasted_iota(jnp.int32, head.shape, 1), 2) == 0
    swapped = jnp.where(even, pltpu.roll(head, 127, 1), pltpu.roll(head, 1, 1))
    return jnp.concatenate([head * cos + swapped * sin, rest], axis=1).astype(BF16)


def attend(query, key, value, k_old, v_old, pos_row, pos_lane, slots):
    n_rows, n_cols = query.shape[0], k_old.shape[0]
    log = slots.bit_length() - 1
    row = lax.broadcasted_iota(jnp.int32, (n_cols, n_rows), 0)
    col = lax.broadcasted_iota(jnp.int32, (n_cols, n_rows), 1)
    hit = ((row >> log) == (col & (GROUP - 1))) & ((row & (slots - 1)) == pos_lane)
    one_hot = jnp.where(hit, 1.0, 0.0)
    written = jnp.sum(one_hot, axis=1, keepdims=True) > 0.5
    one_hot = one_hot.astype(BF16)
    caches = []
    for new, old in ((key, k_old), (value, v_old)):
        placed = jnp.dot(one_hot, new, preferred_element_type=F32)
        caches.append(jnp.where(written, placed, old.astype(F32)).astype(BF16))
    scores = lax.dot_general(query, caches[0], (((1,), (1,)), ((), ())), preferred_element_type=F32) * (query.shape[1] ** -0.5)
    row = lax.broadcasted_iota(jnp.int32, (n_rows, n_cols), 0)
    col = lax.broadcasted_iota(jnp.int32, (n_rows, n_cols), 1)
    visible = ((row & (GROUP - 1)) == (col >> log)) & ((col & (slots - 1)) <= pos_row)
    scores = jnp.where(visible, scores, -jnp.inf)
    exp_scores = jnp.exp(scores - jnp.max(scores, axis=-1, keepdims=True))
    probs = (exp_scores / jnp.sum(exp_scores, axis=-1, keepdims=True)).astype(BF16)
    return jnp.dot(probs, caches[1], preferred_element_type=F32), caches


def decode_kernel(pos_row_ref, pos_lane_ref, cos_ref, sin_ref, gain_ref, bias_ref, b_in_ref, b_out_ref,
                  x_ref, k_ref, v_ref, wq_ref, wk_ref, wv_ref, w_in_ref, w_o_ref, w_out_ref,
                  out_ref, k_out_ref, v_out_ref,
                  w_qkv, w_in, w_cat, qkv, ctx, lhs, cache, hid, pbuf, sib_in, ring_in,
                  x_sem, own_sem, w_sem, cat_sem, cin_sem, cout_sem,
                  sib_s, sib_r, ring_s, ring_r, ag_s, ag_r, agsib_s, agsib_r):
    me = lax.axis_index("tp")
    chip, core = lax.div(me, 2), lax.rem(me, 2)
    pos = ring_of_chip(chip)
    right = {"tp": 2 * chip_of_ring(pos + 1) + core}
    left = {"tp": 2 * chip_of_ring(pos - 1) + core}
    sibling = {"tp": 2 * chip + 1 - core}
    chip_at = {off: chip_of_ring(pos + off) for off in OFFSETS + (-4,)}
    toward = (right, left)
    steps, batch, width = out_ref.shape
    half = batch // HALVES
    rows = steps * half
    part = width // STREAMS
    dim = qkv.shape[3]
    ff = w_in.shape[1]
    slots = cache.shape[3]

    def x_load(h):
        return pltpu.make_async_copy(x_ref.at[:, h * half:(h + 1) * half], out_ref.at[:, h * half:(h + 1) * half], x_sem.at[h])

    def own_load(h):
        return pltpu.make_async_copy(x_ref.at[me, h * half:(h + 1) * half], hid.at[h], own_sem.at[h])

    def in_loads(layer):
        return [pltpu.make_async_copy(w.at[layer], w_qkv.at[i], w_sem.at[i]) for i, w in enumerate((wq_ref, wk_ref, wv_ref))] + [
            pltpu.make_async_copy(w_in_ref.at[layer], w_in, w_sem.at[3])]

    def cat_loads(layer):
        loads = []
        for i in range(STREAMS):
            cols = slice(i * part, (i + 1) * part)
            loads.append(pltpu.make_async_copy(w_o_ref.at[layer, :, cols], w_cat.at[i, 0:dim, :], cat_sem.at[2 * i]))
            loads.append(pltpu.make_async_copy(w_out_ref.at[layer, :, cols], w_cat.at[i, dim:, :], cat_sem.at[2 * i + 1]))
        return loads

    def cache_loads(layer, h):
        return [pltpu.make_async_copy(ref.at[layer, h * half:(h + 1) * half], cache.at[h, i], cin_sem.at[h, i])
                for i, ref in enumerate((k_ref, v_ref))]

    def cache_stores(layer, h):
        return [pltpu.make_async_copy(cache.at[h, i], ref.at[layer, h * half:(h + 1) * half], cout_sem.at[h, i])
                for i, ref in enumerate((k_out_ref, v_out_ref))]

    def start(copies):
        for copy in copies:
            copy.start()

    def wait(copies):
        for copy in copies:
            copy.wait()

    def remote(src, dst, send_sem, recv_sem, device):
        return pltpu.make_async_remote_copy(src_ref=src, dst_ref=dst, send_sem=send_sem, recv_sem=recv_sem,
                                            device_id=device, device_id_type=pl.DeviceIdType.MESH)

    def sib_copy(h, owner, i):
        return remote(pbuf.at[h, owner, i, 1 - core], sib_in.at[h, owner, i], sib_s.at[h, owner, i], sib_r.at[h, owner, i], sibling)

    def ring_copy(h, way, hop, i):
        owner = chip_at[4 - hop] if way == 0 else chip_at[hop - 4]
        return remote(pbuf.at[h, owner, i, core], ring_in.at[h, way, hop, i], ring_s.at[h, way, hop, i],
                      ring_r.at[h, way, hop, i], toward[way])

    def landing(h, off, i):
        return out_ref.at[2 * chip_at[off] + core, h * half:(h + 1) * half, i * part:(i + 1) * part]

    def gather_copy(h, way, hop, i):
        place = landing(h, (1 - hop) if way == 0 else (hop - 1), i)
        return remote(place, place, ag_s.at[h, way, hop - 1, i], ag_r.at[h, way, hop - 1, i], toward[way])

    def gather_sib(h, off, i):
        place = landing(h, off, i)
        at = OFFSETS.index(off)
        return remote(place, place, agsib_s.at[h, at, i], agsib_r.at[h, at, i], sibling)

    def has_fourth(way, i):
        return (i < STREAMS // 2) == (way == 0)

    def add_up(h, owner, i, ring_terms):
        total = pbuf[h, owner, i, core].astype(F32) + sib_in[h, owner, i].astype(F32)
        for term in ring_terms:
            total = total + term.astype(F32)
        return total

    def rs_hop(h, hop):
        order = list(range(STREAMS))
        if hop == 1:
            order = order[STREAMS // 2:] + order[:STREAMS // 2]
        for i in order:
            for way in range(2):
                k = i if way == 0 else STREAMS - 1 - i
                if hop == 0 and not has_fourth(way, k):
                    continue
                owner = chip_at[4 - hop] if way == 0 else chip_at[hop - 4]
                sib_copy(h, owner, k).wait_recv()
                terms = []
                if hop > 1 or (hop == 1 and has_fourth(way, k)):
                    ring_copy(h, way, hop - 1, k).wait_recv()
                    terms.append(ring_in[h, way, hop - 1, k])
                pbuf[h, owner, k, core] = add_up(h, owner, k, terms).astype(BF16)
                ring_copy(h, way, hop, k).start()

    def finish(layer, h):
        mine = slice(h * half, (h + 1) * half)
        if layer == 0:
            own_load(h).wait()
        for i in range(STREAMS):
            cols = slice(i * part, (i + 1) * part)
            sib_copy(h, chip, i).wait_recv()
            terms = []
            for way in range(2):
                ring_copy(h, way, 3, i).wait_recv()
                terms.append(ring_in[h, way, 3, i])
            total = hid[h, :, cols].astype(F32) + add_up(h, chip, i, terms) + b_out_ref[layer:layer + 1, cols].astype(F32)
            if layer + 1 < LAYERS:
                hid[h, :, cols] = total.astype(BF16)
            else:
                out_ref[me, mine, cols] = total.astype(BF16)
        if layer + 1 < LAYERS:
            def store(col, value):
                out_ref[me, mine, col:col + 128] = value

            norm_rows(lambda col: hid[h, :, col:col + 128], store, gain_ref, bias_ref, layer + 1, width)
        for i in range(STREAMS):
            for way in range(2):
                gather_copy(h, way, 1, i).start()
            gather_sib(h, 0, i).start()

    def ag_hop(h, hop):
        for i in range(STREAMS):
            for way in range(2):
                k = i if way == 0 else STREAMS - 1 - i
                gather_copy(h, way, hop - 1, k).wait_recv()
                if hop < 4 or has_fourth(way, k):
                    gather_copy(h, way, hop, k).start()
                gather_sib(h, (1 - hop) if way == 0 else (hop - 1), k).start()

    def ag_end(h):
        for i in range(STREAMS):
            gather_copy(h, 0 if has_fourth(0, i) else 1, 4, i).wait_recv()
            gather_sib(h, 4, i).start()
        for i in range(STREAMS):
            for off in OFFSETS:
                gather_sib(h, off, i).wait_recv()
                gather_sib(h, off, i).wait_send()
            for chip_index in range(CHIPS):
                sib_copy(h, chip_index, i).wait_send()
            for way in range(2):
                for hop in range(4):
                    if hop > 0 or has_fourth(way, i):
                        ring_copy(h, way, hop, i).wait_send()
                    if hop < 3 or has_fourth(way, i):
                        gather_copy(h, way, hop + 1, i).wait_send()

    def norm_first(h):
        x_load(h).wait()
        group = 64 // half

        def body(g, carry):
            ts, mine = pl.ds(g * group, group), slice(h * half, (h + 1) * half)

            def load(col):
                return out_ref[ts, mine, col:col + 128].reshape(group * half, 128)

            def store(col, value):
                out_ref[ts, mine, col:col + 128] = value.reshape(group, half, 128)

            norm_rows(load, store, gain_ref, bias_ref, 0, width)
            return carry

        lax.fori_loop(0, steps // group, body, 0)

    def product(h, w_cols):
        total = None
        depth = width // 4
        for i in range(4):
            piece = out_ref[:, h * half:(h + 1) * half, i * depth:(i + 1) * depth].reshape(rows, depth)
            term = jnp.dot(piece, w_cols(i * depth, depth), preferred_element_type=F32)
            total = term if total is None else total + term
        return total

    def put_qkv(i, value):
        qkv[i] = value.astype(F32).reshape(steps, half, dim)

    def do_qk(layer, h):
        if h == 0:
            wait(in_loads(layer)[:3])

        def body(i, carry):
            table = slice(h * rows, (h + 1) * rows)
            put_qkv(i, rotate(product(h, lambda k0, depth: w_qkv[i, k0:k0 + depth, :]), cos_ref[table], sin_ref[table]))
            return carry

        lax.fori_loop(0, 2, body, 0)

    def do_v(layer, h):
        put_qkv(2, product(h, lambda k0, depth: w_qkv[2, k0:k0 + depth, :]).astype(BF16))

    def do_in(layer, h, lo, hi):
        tile = min(512, ff)
        if lo == 0 and h == 0:
            wait(in_loads(layer)[3:])

        def body(n, carry):
            cols = pl.ds(pl.multiple_of(n * tile, tile), tile)
            pre = product(h, lambda k0, depth: w_in[k0:k0 + depth, cols]) + b_in_ref[layer:layer + 1, cols].astype(F32)
            lhs[:, pl.ds(pl.multiple_of(dim + n * tile, 128), tile)] = jax.nn.gelu(pre, approximate=True).astype(BF16)
            return carry

        count = ff // tile
        lax.fori_loop(lo * count // 2, hi * count // 2, body, 0)
        if hi == 2 and h == HALVES - 1 and layer + 1 < LAYERS:
            start(in_loads(layer + 1))

    def do_attention(layer, h, lo, hi):
        if lo == 0:
            wait(cache_loads(layer, h))
        count = half // GROUP

        def body(g, carry):
            seqs = pl.ds(pl.multiple_of(g * GROUP, GROUP), GROUP)
            flat = lambda i: qkv[i, :, seqs, :].reshape(steps * GROUP, dim).astype(BF16)
            old = [cache[h, i, seqs].reshape(GROUP * slots, dim) for i in range(2)]
            context, caches = attend(flat(0), flat(1), flat(2), old[0], old[1],
                                     pos_row_ref[h * count + g], pos_lane_ref[h * count + g], slots)
            for i in range(2):
                cache[h, i, seqs] = caches[i].reshape(GROUP, slots, dim)
            ctx[:, seqs, :] = context.reshape(steps, GROUP, dim)
            return carry

        lax.fori_loop(lo * count // 2, hi * count // 2, body, 0)
        if hi == 2:
            start(cache_stores(layer, h))
            lhs[:, :dim] = ctx[...].reshape(rows, dim).astype(BF16)

    def do_partials(layer, h, lo, hi):
        tile = min(512, part)
        per = part // tile
        if lo == 0 and h == 0:
            wait(cat_loads(layer))

        def body(n, carry):
            i = lax.div(n, per)
            cols = pl.ds(pl.multiple_of(lax.rem(n, per) * tile, tile), tile)
            value = jnp.dot(lhs[...], w_cat[i, :, cols], preferred_element_type=F32).astype(BF16)
            for owner in range(CHIPS):
                for c in range(2):
                    at = (2 * owner + c) * half
                    pbuf[h, owner, i, c, :, cols] = value[at:at + half]
            return carry

        count = STREAMS * per
        lax.fori_loop(lo * count // 2, hi * count // 2, body, 0)
        for i in range(lo * STREAMS // 2, hi * STREAMS // 2):
            for off in (4, 3, -3, 2, -2, 1, -1, 0):
                sib_copy(h, chip_at[off], i).start()
        if hi == 2 and h == HALVES - 1 and layer + 1 < LAYERS:
            start(cat_loads(layer + 1))

    def next_caches(layer, h):
        wait(cache_stores(layer - 1, h))
        start(cache_loads(layer, h))

    def compute(layer, h):
        pieces = []
        if layer == 0:
            pieces.append((4.2, lambda: norm_first(h)))
        else:
            pieces.append((0.0, lambda: next_caches(layer, h)))
        pieces += [(2.6, lambda: do_qk(layer, h)), (1.3, lambda: do_v(layer, h)),
                   (2.6, lambda: do_in(layer, h, 0, 1)), (2.6, lambda: do_in(layer, h, 1, 2)),
                   (1.8, lambda: do_attention(layer, h, 0, 1)), (1.8, lambda: do_attention(layer, h, 1, 2)),
                   (3.4, lambda: do_partials(layer, h, 0, 1)), (3.4, lambda: do_partials(layer, h, 1, 2))]
        return pieces

    def services(layer, h):
        return [lambda hop=hop: rs_hop(h, hop) for hop in range(4)] + [lambda: finish(layer, h)] + [
            lambda hop=hop: ag_hop(h, hop) for hop in range(2, 5)] + [lambda: ag_end(h)]

    x_load(0).start()
    start(in_loads(0))
    x_load(1).start()
    start(cat_loads(0))
    for h in range(HALVES):
        start(cache_loads(0, h))
        own_load(h).start()
    barrier = pltpu.get_barrier_semaphore()
    for peer in (left, right, sibling):
        pl.semaphore_signal(barrier, inc=1, device_id=peer, device_id_type=pl.DeviceIdType.MESH)
    pl.semaphore_wait(barrier, 3)

    for _, piece in compute(0, 0):
        piece()
    phases = [(0, 0), (0, 1), (1, 0), (1, 1)]
    ahead = 2
    todo = services(*phases[0])
    for at, (layer, h) in enumerate(phases):
        follow = phases[at + 1] if at + 1 < len(phases) else None
        pieces = compute(*follow) if follow else []
        nxt = services(*follow) if follow else []
        tail, todo = todo[-ahead:], todo[:-ahead]
        for service in todo:
            service()
            spent = 0.0
            while pieces and spent < SERVICE_US:
                cost, piece = pieces.pop(0)
                piece()
                spent += cost
        for _, piece in pieces:
            piece()
        for service in tail:
            if nxt:
                nxt.pop(0)()
            service()
        todo = nxt
    for h in range(HALVES):
        wait(cache_stores(LAYERS - 1, h))


def decode_shard(x_steps, cur_len, k_cache, v_cache, ln_gain, ln_bias, w_q, w_k, w_v, w_o, w_in, b_in, w_out, b_out):
    n_layers, batch, slots, _, dim = k_cache.shape
    steps, _, width = x_steps.shape
    ff = w_in.shape[2]
    half = batch // HALVES
    rows, part = steps * half, width // STREAMS
    pos = cur_len[None, :] + jnp.arange(steps, dtype=jnp.int32)[:, None]
    by_half = pos.reshape(steps, HALVES, half).transpose(1, 0, 2).reshape(HALVES * rows)
    cos, sin = rotary_tables(by_half)
    groups = batch // GROUP
    grouped = pos.reshape(steps, groups, GROUP).transpose(1, 0, 2).reshape(groups, steps * GROUP)
    pos_row, pos_lane = grouped[:, :, None], grouped[:, None, :]
    k_old, v_old = k_cache.reshape(n_layers, batch, slots, dim), v_cache.reshape(n_layers, batch, slots, dim)
    vmem, hbm = pl.BlockSpec(memory_space=pltpu.VMEM), pl.BlockSpec(memory_space=pl.ANY)
    dma = pltpu.SemaphoreType.DMA
    out, k_new, v_new = pl.pallas_call(
        decode_kernel,
        in_specs=[vmem] * 8 + [hbm] * 9,
        out_specs=[vmem, hbm, hbm],
        out_shape=[pltpu.VMEM((steps, batch, width), BF16)] + [jax.ShapeDtypeStruct(k_old.shape, BF16)] * 2,
        scratch_shapes=[
            pltpu.VMEM((3, width, dim), BF16), pltpu.VMEM((width, ff), BF16), pltpu.VMEM((STREAMS, dim + ff, part), BF16),
            pltpu.VMEM((3, steps, half, dim), F32), pltpu.VMEM((steps, half, dim), F32), pltpu.VMEM((rows, dim + ff), BF16),
            pltpu.VMEM((HALVES, 2, half, slots, dim), BF16), pltpu.VMEM((HALVES, half, width), BF16),
            pltpu.VMEM((HALVES, CHIPS, STREAMS, 2, half, part), BF16), pltpu.VMEM((HALVES, CHIPS, STREAMS, half, part), BF16),
            pltpu.VMEM((HALVES, 2, 4, STREAMS, half, part), BF16),
            dma((HALVES,)), dma((HALVES,)), dma((4,)), dma((2 * STREAMS,)), dma((HALVES, 2)), dma((HALVES, 2)),
            dma((HALVES, CHIPS, STREAMS)), dma((HALVES, CHIPS, STREAMS)),
            dma((HALVES, 2, 4, STREAMS)), dma((HALVES, 2, 4, STREAMS)), dma((HALVES, 2, 4, STREAMS)), dma((HALVES, 2, 4, STREAMS)),
            dma((HALVES, CHIPS, STREAMS)), dma((HALVES, CHIPS, STREAMS))],
        compiler_params=pltpu.CompilerParams(collective_id=0, has_side_effects=True,
                                             vmem_limit_bytes=VMEM_LIMIT - 2 * steps * batch * width),
        name="decode",
    )(pos_row, pos_lane, cos, sin, ln_gain, ln_bias, b_in, b_out, x_steps, k_old, v_old, w_q, w_k, w_v, w_in, w_o, w_out)
    return out, k_new.reshape(k_cache.shape), v_new.reshape(v_cache.shape)


def rotary_tables(positions):
    inv_freq = 1.0 / (10000.0 ** (jnp.arange(0, ROT_DIM, 2).astype(F32) / ROT_DIM))
    angles = positions.astype(F32)[:, None] * inv_freq[None, :]
    cos = jnp.repeat(jnp.cos(angles), 2, axis=1)
    sin = jnp.repeat(jnp.sin(angles), 2, axis=1) * jnp.where(jnp.arange(ROT_DIM) % 2 == 0, -1.0, 1.0)
    rest = 128 - ROT_DIM
    return jnp.pad(cos, ((0, 0), (0, rest)), constant_values=1.0), jnp.pad(sin, ((0, 0), (0, rest)))


def solution(mesh):
    cache_spec = P(None, "dp", None, "tp", None)
    in_specs = (P(None, "dp", None), P("dp"), cache_spec, cache_spec, P(None, None), P(None, None),
                P(None, None, "tp"), P(None, None, "tp"), P(None, None, "tp"), P(None, "tp", None),
                P(None, None, "tp"), P(None, "tp"), P(None, "tp", None), P(None, None))
    out_specs = (P(None, "dp", None), cache_spec, cache_spec)
    return jax.shard_map(decode_shard, mesh=mesh, in_specs=in_specs, out_specs=out_specs, check_vma=False)
```

```python
import jax
import jax.numpy as jnp
from jax import lax
from jax.experimental import pallas as pl
from jax.experimental.pallas import tpu as pltpu
from jax.sharding import PartitionSpec as P

ROT_DIM = 64
LN_EPS = 1e-5
TP = 16
CHIPS = 8
STREAMS = 4
BF16 = jnp.bfloat16
F32 = jnp.float32
VMEM_LIMIT = 67_000_000
OFFSETS = (0, -1, 1, -2, 2, -3, 3, 4)
HALVES = 2
LAYERS = 2
GROUP = 8
ORDER = (
    (0, 0, 0, 0), (0, 0, 0, 1), (0, 0, 1, 2), (0, 0, 1, 3), (4, 1, 0, 0), (0, 0, 1, 0), (0, 0, 1, 1), (4, 1, 1, 0), (4, 1, 2, 0),
    (0, 0, 2, 0), (0, 0, 2, 1), (0, 0, 2, 2), (0, 0, 2, 3), (4, 1, 3, 0), (0, 0, 3, 0), (0, 0, 3, 1), (0, 0, 3, 2), (0, 0, 3, 3),
    (4, 1, 4, 0), (4, 1, 5, 0), (4, 1, 6, 0), (1, 0, 0, 0), (4, 1, 7, 0), (4, 1, 8, 0), (2, 0, 2, 0), (2, 0, 2, 1), (2, 0, 2, 2),
    (2, 0, 2, 3), (2, 0, 3, 0), (2, 0, 3, 1), (2, 0, 3, 2), (2, 0, 3, 3), (0, 1, 0, 0), (0, 1, 0, 1), (0, 1, 1, 2), (0, 1, 1, 3),
    (2, 0, 4, 0), (2, 0, 4, 1), (2, 0, 4, 2), (2, 0, 4, 3), (0, 1, 1, 0), (0, 1, 1, 1), (3, 0, 0, 0), (0, 1, 2, 0), (0, 1, 2, 1),
    (0, 1, 2, 2), (0, 1, 2, 3), (4, 2, 0, 0), (0, 1, 3, 0), (0, 1, 3, 1), (4, 2, 1, 0), (0, 1, 3, 2), (0, 1, 3, 3), (4, 2, 2, 0),
    (4, 2, 3, 0), (1, 1, 0, 0), (4, 2, 4, 0), (4, 2, 5, 0), (4, 2, 6, 0), (2, 1, 2, 0), (2, 1, 2, 1), (2, 1, 2, 2), (2, 1, 2, 3),
    (4, 2, 7, 0), (2, 1, 3, 0), (2, 1, 3, 1), (2, 1, 3, 2), (2, 1, 3, 3), (0, 2, 0, 0), (0, 2, 0, 1), (0, 2, 1, 2), (0, 2, 1, 3),
    (2, 1, 4, 0), (2, 1, 4, 1), (2, 1, 4, 2), (2, 1, 4, 3), (0, 2, 1, 0), (0, 2, 1, 1), (3, 1, 0, 0), (0, 2, 2, 0), (0, 2, 2, 1),
    (0, 2, 2, 2), (0, 2, 2, 3), (4, 3, 0, 0), (0, 2, 3, 0), (0, 2, 3, 1), (4, 3, 1, 0), (0, 2, 3, 2), (0, 2, 3, 3), (4, 3, 2, 0),
    (4, 3, 3, 0), (1, 2, 0, 0), (4, 3, 4, 0), (4, 3, 5, 0), (4, 3, 6, 0), (2, 2, 2, 0), (2, 2, 2, 1), (2, 2, 2, 2), (2, 2, 2, 3),
    (4, 3, 7, 0), (2, 2, 3, 0), (2, 2, 3, 1), (2, 2, 3, 2), (2, 2, 3, 3), (0, 3, 0, 0), (0, 3, 0, 1), (0, 3, 1, 2), (0, 3, 1, 3),
    (2, 2, 4, 0), (2, 2, 4, 1), (2, 2, 4, 2), (2, 2, 4, 3), (0, 3, 1, 0), (0, 3, 1, 1), (3, 2, 0, 0), (0, 3, 2, 0), (0, 3, 2, 1),
    (0, 3, 2, 2), (0, 3, 2, 3), (0, 3, 3, 0), (0, 3, 3, 1), (0, 3, 3, 2), (0, 3, 3, 3), (1, 3, 0, 0), (2, 3, 2, 0), (2, 3, 2, 1),
    (2, 3, 2, 2), (2, 3, 2, 3), (2, 3, 3, 0), (2, 3, 3, 1), (2, 3, 3, 2), (2, 3, 3, 3), (2, 3, 4, 0), (2, 3, 4, 1), (2, 3, 4, 2),
    (2, 3, 4, 3), (3, 3, 0, 0),
)


def ring_of_chip(chip):
    z, y = lax.div(chip, 2), lax.rem(chip, 2)
    return z + y * (7 - 2 * z)


def chip_of_ring(pos):
    pos = lax.rem(pos + 2 * CHIPS, CHIPS)
    y = lax.div(pos, 4)
    z = pos + y * (7 - 2 * pos)
    return 2 * z + y


def norm_rows(load, store, gain_ref, bias_ref, layer, width):
    starts = range(0, width, 128)
    total = load(0).astype(F32)
    for col in starts[1:]:
        total = total + load(col).astype(F32)
    mean = jnp.sum(total, axis=-1, keepdims=True) * (1.0 / width)
    square = jnp.zeros_like(total)
    for col in starts:
        centered = load(col).astype(F32) - mean
        square = square + centered * centered
    scale = lax.rsqrt(jnp.sum(square, axis=-1, keepdims=True) * (1.0 / width) + LN_EPS)
    for col in starts:
        gain = gain_ref[layer:layer + 1, col:col + 128].astype(F32)
        bias = bias_ref[layer:layer + 1, col:col + 128].astype(F32)
        store(col, ((load(col).astype(F32) - mean) * scale * gain + bias).astype(BF16))


def rotate(vec, cos, sin):
    head, rest = vec[:, :128], vec[:, 128:]
    even = lax.rem(lax.broadcasted_iota(jnp.int32, head.shape, 1), 2) == 0
    swapped = jnp.where(even, pltpu.roll(head, 127, 1), pltpu.roll(head, 1, 1))
    return jnp.concatenate([head * cos + swapped * sin, rest], axis=1).astype(BF16)


def attend(query, key, value, k_old, v_old, pos_row, pos_lane, slots):
    n_rows, n_cols = query.shape[0], k_old.shape[0]
    log = slots.bit_length() - 1
    row = lax.broadcasted_iota(jnp.int32, (n_cols, n_rows), 0)
    col = lax.broadcasted_iota(jnp.int32, (n_cols, n_rows), 1)
    hit = ((row >> log) == (col & (GROUP - 1))) & ((row & (slots - 1)) == pos_lane)
    one_hot = jnp.where(hit, 1.0, 0.0)
    written = jnp.sum(one_hot, axis=1, keepdims=True) > 0.5
    one_hot = one_hot.astype(BF16)
    caches = []
    for new, old in ((key, k_old), (value, v_old)):
        placed = jnp.dot(one_hot, new, preferred_element_type=F32)
        caches.append(jnp.where(written, placed, old.astype(F32)).astype(BF16))
    scores = lax.dot_general(query, caches[0], (((1,), (1,)), ((), ())), preferred_element_type=F32) * (query.shape[1] ** -0.5)
    row = lax.broadcasted_iota(jnp.int32, (n_rows, n_cols), 0)
    col = lax.broadcasted_iota(jnp.int32, (n_rows, n_cols), 1)
    visible = ((row & (GROUP - 1)) == (col >> log)) & ((col & (slots - 1)) <= pos_row)
    scores = jnp.where(visible, scores, -jnp.inf)
    exp_scores = jnp.exp(scores - jnp.max(scores, axis=-1, keepdims=True))
    probs = (exp_scores / jnp.sum(exp_scores, axis=-1, keepdims=True)).astype(BF16)
    return jnp.dot(probs, caches[1], preferred_element_type=F32), caches


def decode_kernel(pos_row_ref, pos_lane_ref, cos_ref, sin_ref, gain_ref, bias_ref, b_in_ref, b_out_ref,
                  x_ref, k_ref, v_ref, wq_ref, wk_ref, wv_ref, w_in_ref, w_o_ref, w_out_ref,
                  out_ref, k_out_ref, v_out_ref,
                  w_qkv, w_in, w_cat, qkv, ctx, lhs, cache, hid, pbuf, sib_in, ring_in,
                  x_sem, own_sem, w_sem, cat_sem, cin_sem, cout_sem,
                  sib_s, sib_r, ring_s, ring_r, ag_s, ag_r, agsib_s, agsib_r):
    me = lax.axis_index("tp")
    chip, core = lax.div(me, 2), lax.rem(me, 2)
    pos = ring_of_chip(chip)
    right = {"tp": 2 * chip_of_ring(pos + 1) + core}
    left = {"tp": 2 * chip_of_ring(pos - 1) + core}
    sibling = {"tp": 2 * chip + 1 - core}
    chip_at = {off: chip_of_ring(pos + off) for off in OFFSETS + (-4,)}
    toward = (right, left)
    steps, batch, width = out_ref.shape
    half = batch // HALVES
    rows = steps * half
    part = width // STREAMS
    dim = qkv.shape[3]
    ff = w_in.shape[1]
    slots = cache.shape[3]

    def x_load(h):
        return pltpu.make_async_copy(x_ref.at[:, h * half:(h + 1) * half], out_ref.at[:, h * half:(h + 1) * half], x_sem.at[h])

    def own_load(h):
        return pltpu.make_async_copy(x_ref.at[me, h * half:(h + 1) * half], hid.at[h], own_sem.at[h])

    def in_loads(layer):
        return [pltpu.make_async_copy(w.at[layer], w_qkv.at[i], w_sem.at[i]) for i, w in enumerate((wq_ref, wk_ref, wv_ref))] + [
            pltpu.make_async_copy(w_in_ref.at[layer], w_in, w_sem.at[3])]

    def cat_loads(layer):
        loads = []
        for i in range(STREAMS):
            cols = slice(i * part, (i + 1) * part)
            loads.append(pltpu.make_async_copy(w_o_ref.at[layer, :, cols], w_cat.at[i, 0:dim, :], cat_sem.at[2 * i]))
            loads.append(pltpu.make_async_copy(w_out_ref.at[layer, :, cols], w_cat.at[i, dim:, :], cat_sem.at[2 * i + 1]))
        return loads

    def cache_loads(layer, h):
        return [pltpu.make_async_copy(ref.at[layer, h * half:(h + 1) * half], cache.at[h, i], cin_sem.at[h, i])
                for i, ref in enumerate((k_ref, v_ref))]

    def cache_stores(layer, h):
        return [pltpu.make_async_copy(cache.at[h, i], ref.at[layer, h * half:(h + 1) * half], cout_sem.at[h, i])
                for i, ref in enumerate((k_out_ref, v_out_ref))]

    def start(copies):
        for copy in copies:
            copy.start()

    def wait(copies):
        for copy in copies:
            copy.wait()

    def remote(src, dst, send_sem, recv_sem, device):
        return pltpu.make_async_remote_copy(src_ref=src, dst_ref=dst, send_sem=send_sem, recv_sem=recv_sem,
                                            device_id=device, device_id_type=pl.DeviceIdType.MESH)

    def sib_copy(h, owner, i):
        return remote(pbuf.at[h, owner, i, 1 - core], sib_in.at[h, owner, i], sib_s.at[h, owner, i], sib_r.at[h, owner, i], sibling)

    def ring_copy(h, way, hop, i):
        owner = chip_at[4 - hop] if way == 0 else chip_at[hop - 4]
        return remote(pbuf.at[h, owner, i, core], ring_in.at[h, way, hop, i], ring_s.at[h, way, hop, i],
                      ring_r.at[h, way, hop, i], toward[way])

    def landing(h, off, i):
        return out_ref.at[2 * chip_at[off] + core, h * half:(h + 1) * half, i * part:(i + 1) * part]

    def gather_copy(h, way, hop, i):
        place = landing(h, (1 - hop) if way == 0 else (hop - 1), i)
        return remote(place, place, ag_s.at[h, way, hop - 1, i], ag_r.at[h, way, hop - 1, i], toward[way])

    def gather_sib(h, off, i):
        place = landing(h, off, i)
        at = OFFSETS.index(off)
        return remote(place, place, agsib_s.at[h, at, i], agsib_r.at[h, at, i], sibling)

    def has_fourth(way, i):
        return (i < STREAMS // 2) == (way == 0)

    def add_up(h, owner, i, ring_terms):
        total = pbuf[h, owner, i, core].astype(F32) + sib_in[h, owner, i].astype(F32)
        for term in ring_terms:
            total = total + term.astype(F32)
        return total

    def rs_item(h, hop, i):
        for way in range(2):
            k = i if way == 0 else STREAMS - 1 - i
            if hop == 0 and not has_fourth(way, k):
                continue
            owner = chip_at[4 - hop] if way == 0 else chip_at[hop - 4]
            sib_copy(h, owner, k).wait_recv()
            terms = []
            if hop > 1 or (hop == 1 and has_fourth(way, k)):
                ring_copy(h, way, hop - 1, k).wait_recv()
                terms.append(ring_in[h, way, hop - 1, k])
            pbuf[h, owner, k, core] = add_up(h, owner, k, terms).astype(BF16)
            ring_copy(h, way, hop, k).start()

    def finish(layer, h):
        mine = slice(h * half, (h + 1) * half)
        if layer == 0:
            own_load(h).wait()
        for i in range(STREAMS):
            cols = slice(i * part, (i + 1) * part)
            sib_copy(h, chip, i).wait_recv()
            terms = []
            for way in range(2):
                ring_copy(h, way, 3, i).wait_recv()
                terms.append(ring_in[h, way, 3, i])
            total = hid[h, :, cols].astype(F32) + add_up(h, chip, i, terms) + b_out_ref[layer:layer + 1, cols].astype(F32)
            if layer + 1 < LAYERS:
                hid[h, :, cols] = total.astype(BF16)
            else:
                out_ref[me, mine, cols] = total.astype(BF16)
        if layer + 1 < LAYERS:
            def store(col, value):
                out_ref[me, mine, col:col + 128] = value

            norm_rows(lambda col: hid[h, :, col:col + 128], store, gain_ref, bias_ref, layer + 1, width)
        for i in range(STREAMS):
            for way in range(2):
                gather_copy(h, way, 1, i).start()
            gather_sib(h, 0, i).start()

    def ag_item(h, hop, i):
        for way in range(2):
            k = i if way == 0 else STREAMS - 1 - i
            gather_copy(h, way, hop - 1, k).wait_recv()
            if hop < 4 or has_fourth(way, k):
                gather_copy(h, way, hop, k).start()
            gather_sib(h, (1 - hop) if way == 0 else (hop - 1), k).start()

    def ag_end(h):
        for i in range(STREAMS):
            gather_copy(h, 0 if has_fourth(0, i) else 1, 4, i).wait_recv()
            gather_sib(h, 4, i).start()
        for i in range(STREAMS):
            for off in OFFSETS:
                gather_sib(h, off, i).wait_recv()
                gather_sib(h, off, i).wait_send()
            for chip_index in range(CHIPS):
                sib_copy(h, chip_index, i).wait_send()
            for way in range(2):
                for hop in range(4):
                    if hop > 0 or has_fourth(way, i):
                        ring_copy(h, way, hop, i).wait_send()
                    if hop < 3 or has_fourth(way, i):
                        gather_copy(h, way, hop + 1, i).wait_send()

    def norm_first(h, lo, hi):
        if lo == 0:
            x_load(h).wait()
        group = 64 // half

        def body(g, carry):
            ts, mine = pl.ds(g * group, group), slice(h * half, (h + 1) * half)

            def load(col):
                return out_ref[ts, mine, col:col + 128].reshape(group * half, 128)

            def store(col, value):
                out_ref[ts, mine, col:col + 128] = value.reshape(group, half, 128)

            norm_rows(load, store, gain_ref, bias_ref, 0, width)
            return carry

        count = steps // group
        lax.fori_loop(lo * count // 2, hi * count // 2, body, 0)

    def product(h, w_cols):
        total = None
        depth = width // 4
        for i in range(4):
            piece = out_ref[:, h * half:(h + 1) * half, i * depth:(i + 1) * depth].reshape(rows, depth)
            term = jnp.dot(piece, w_cols(i * depth, depth), preferred_element_type=F32)
            total = term if total is None else total + term
        return total

    def put_qkv(i, value):
        qkv[i] = value.astype(F32).reshape(steps, half, dim)

    def do_qk(layer, h, lo, hi):
        if h == 0 and lo == 0:
            wait(in_loads(layer)[:3])

        def body(i, carry):
            table = slice(h * rows, (h + 1) * rows)
            put_qkv(i, rotate(product(h, lambda k0, depth: w_qkv[i, k0:k0 + depth, :]), cos_ref[table], sin_ref[table]))
            return carry

        lax.fori_loop(lo, hi, body, 0)

    def do_v(layer, h):
        put_qkv(2, product(h, lambda k0, depth: w_qkv[2, k0:k0 + depth, :]).astype(BF16))

    def do_in(layer, h, lo, hi):
        tile = min(512, ff)
        if lo == 0 and h == 0:
            wait(in_loads(layer)[3:])

        def body(n, carry):
            cols = pl.ds(pl.multiple_of(n * tile, tile), tile)
            pre = product(h, lambda k0, depth: w_in[k0:k0 + depth, cols]) + b_in_ref[layer:layer + 1, cols].astype(F32)
            lhs[:, pl.ds(pl.multiple_of(dim + n * tile, 128), tile)] = jax.nn.gelu(pre, approximate=True).astype(BF16)
            return carry

        count = ff // tile
        lax.fori_loop(lo * count // 2, hi * count // 2, body, 0)
        if hi == 2 and h == HALVES - 1 and layer + 1 < LAYERS:
            start(in_loads(layer + 1))

    def do_attention(layer, h, lo, hi):
        if lo == 0:
            wait(cache_loads(layer, h))
        count = half // GROUP

        def body(g, carry):
            seqs = pl.ds(pl.multiple_of(g * GROUP, GROUP), GROUP)
            flat = lambda i: qkv[i, :, seqs, :].reshape(steps * GROUP, dim).astype(BF16)
            old = [cache[h, i, seqs].reshape(GROUP * slots, dim) for i in range(2)]
            context, caches = attend(flat(0), flat(1), flat(2), old[0], old[1],
                                     pos_row_ref[h * count + g], pos_lane_ref[h * count + g], slots)
            for i in range(2):
                cache[h, i, seqs] = caches[i].reshape(GROUP, slots, dim)
            ctx[:, seqs, :] = context.reshape(steps, GROUP, dim)
            return carry

        lax.fori_loop(lo * count // 4, hi * count // 4, body, 0)
        if hi == 4:
            start(cache_stores(layer, h))
            lhs[:, :dim] = ctx[...].reshape(rows, dim).astype(BF16)

    def do_partials(layer, h, lo, hi):
        tile = min(512, part)
        per = part // tile
        if lo == 0 and h == 0:
            wait(cat_loads(layer))

        def body(n, carry):
            i = lax.div(n, per)
            cols = pl.ds(pl.multiple_of(lax.rem(n, per) * tile, tile), tile)
            value = jnp.dot(lhs[...], w_cat[i, :, cols], preferred_element_type=F32).astype(BF16)
            for owner in range(CHIPS):
                for c in range(2):
                    at = (2 * owner + c) * half
                    pbuf[h, owner, i, c, :, cols] = value[at:at + half]
            return carry

        lax.fori_loop(lo * per, hi * per, body, 0)
        for i in range(lo, hi):
            for off in (4, 3, -3, 2, -2, 1, -1, 0):
                sib_copy(h, chip_at[off], i).start()
        if hi == STREAMS and h == HALVES - 1 and layer + 1 < LAYERS:
            start(cat_loads(layer + 1))

    def next_caches(layer, h):
        wait(cache_stores(layer - 1, h))
        start(cache_loads(layer, h))

    def first_work():
        norm_first(0, 0, 2)
        do_qk(0, 0, 0, 2)
        do_v(0, 0)
        do_in(0, 0, 0, 2)
        do_attention(0, 0, 0, 4)
        do_partials(0, 0, 0, STREAMS)

    def work(layer, h):
        pieces = [lambda: norm_first(h, 0, 2)] if layer == 0 else []

        def first_qk():
            if layer > 0:
                next_caches(layer, h)
            do_qk(layer, h, 0, 2)

        pieces += [first_qk, lambda: do_v(layer, h)]
        pieces += [lambda i=i: do_in(layer, h, i, i + 1) for i in range(2)]
        pieces += [lambda i=i: do_attention(layer, h, i, i + 2) for i in (0, 2)]
        return pieces + [lambda i=i: do_partials(layer, h, i, i + 2) for i in range(0, STREAMS, 2)]

    x_load(0).start()
    start(in_loads(0))
    x_load(1).start()
    start(cat_loads(0))
    for h in range(HALVES):
        start(cache_loads(0, h))
        own_load(h).start()
    barrier = pltpu.get_barrier_semaphore()
    for peer in (left, right, sibling):
        pl.semaphore_signal(barrier, inc=1, device_id=peer, device_id_type=pl.DeviceIdType.MESH)
    pl.semaphore_wait(barrier, 3)

    first_work()
    phases = [(layer, h) for layer in range(LAYERS) for h in range(HALVES)]
    pieces = [work(*phase) for phase in phases]
    for kind, at, hop, i in ORDER:
        layer, h = phases[at]
        if kind == 0:
            rs_item(h, hop, i)
        elif kind == 1:
            finish(layer, h)
        elif kind == 2:
            ag_item(h, hop, i)
        elif kind == 3:
            ag_end(h)
        else:
            pieces[at][hop]()
    for h in range(HALVES):
        wait(cache_stores(LAYERS - 1, h))


def decode_shard(x_steps, cur_len, k_cache, v_cache, ln_gain, ln_bias, w_q, w_k, w_v, w_o, w_in, b_in, w_out, b_out):
    n_layers, batch, slots, _, dim = k_cache.shape
    steps, _, width = x_steps.shape
    ff = w_in.shape[2]
    half = batch // HALVES
    rows, part = steps * half, width // STREAMS
    pos = cur_len[None, :] + jnp.arange(steps, dtype=jnp.int32)[:, None]
    by_half = pos.reshape(steps, HALVES, half).transpose(1, 0, 2).reshape(HALVES * rows)
    cos, sin = rotary_tables(by_half)
    groups = batch // GROUP
    grouped = pos.reshape(steps, groups, GROUP).transpose(1, 0, 2).reshape(groups, steps * GROUP)
    pos_row, pos_lane = grouped[:, :, None], grouped[:, None, :]
    k_old, v_old = k_cache.reshape(n_layers, batch, slots, dim), v_cache.reshape(n_layers, batch, slots, dim)
    vmem, hbm = pl.BlockSpec(memory_space=pltpu.VMEM), pl.BlockSpec(memory_space=pl.ANY)
    dma = pltpu.SemaphoreType.DMA
    out, k_new, v_new = pl.pallas_call(
        decode_kernel,
        in_specs=[vmem] * 8 + [hbm] * 9,
        out_specs=[vmem, hbm, hbm],
        out_shape=[pltpu.VMEM((steps, batch, width), BF16)] + [jax.ShapeDtypeStruct(k_old.shape, BF16)] * 2,
        scratch_shapes=[
            pltpu.VMEM((3, width, dim), BF16), pltpu.VMEM((width, ff), BF16), pltpu.VMEM((STREAMS, dim + ff, part), BF16),
            pltpu.VMEM((3, steps, half, dim), F32), pltpu.VMEM((steps, half, dim), F32), pltpu.VMEM((rows, dim + ff), BF16),
            pltpu.VMEM((HALVES, 2, half, slots, dim), BF16), pltpu.VMEM((HALVES, half, width), BF16),
            pltpu.VMEM((HALVES, CHIPS, STREAMS, 2, half, part), BF16), pltpu.VMEM((HALVES, CHIPS, STREAMS, half, part), BF16),
            pltpu.VMEM((HALVES, 2, 4, STREAMS, half, part), BF16),
            dma((HALVES,)), dma((HALVES,)), dma((4,)), dma((2 * STREAMS,)), dma((HALVES, 2)), dma((HALVES, 2)),
            dma((HALVES, CHIPS, STREAMS)), dma((HALVES, CHIPS, STREAMS)),
            dma((HALVES, 2, 4, STREAMS)), dma((HALVES, 2, 4, STREAMS)), dma((HALVES, 2, 4, STREAMS)), dma((HALVES, 2, 4, STREAMS)),
            dma((HALVES, CHIPS, STREAMS)), dma((HALVES, CHIPS, STREAMS))],
        compiler_params=pltpu.CompilerParams(collective_id=0, has_side_effects=True,
                                             vmem_limit_bytes=VMEM_LIMIT - 2 * steps * batch * width),
        name="decode",
    )(pos_row, pos_lane, cos, sin, ln_gain, ln_bias, b_in, b_out, x_steps, k_old, v_old, w_q, w_k, w_v, w_in, w_o, w_out)
    return out, k_new.reshape(k_cache.shape), v_new.reshape(v_cache.shape)


def rotary_tables(positions):
    inv_freq = 1.0 / (10000.0 ** (jnp.arange(0, ROT_DIM, 2).astype(F32) / ROT_DIM))
    angles = positions.astype(F32)[:, None] * inv_freq[None, :]
    cos = jnp.repeat(jnp.cos(angles), 2, axis=1)
    sin = jnp.repeat(jnp.sin(angles), 2, axis=1) * jnp.where(jnp.arange(ROT_DIM) % 2 == 0, -1.0, 1.0)
    rest = 128 - ROT_DIM
    return jnp.pad(cos, ((0, 0), (0, rest)), constant_values=1.0), jnp.pad(sin, ((0, 0), (0, rest)))


def solution(mesh):
    cache_spec = P(None, "dp", None, "tp", None)
    in_specs = (P(None, "dp", None), P("dp"), cache_spec, cache_spec, P(None, None), P(None, None),
                P(None, None, "tp"), P(None, None, "tp"), P(None, None, "tp"), P(None, "tp", None),
                P(None, None, "tp"), P(None, "tp"), P(None, "tp", None), P(None, None))
    out_specs = (P(None, "dp", None), cache_spec, cache_spec)
    return jax.shard_map(decode_shard, mesh=mesh, in_specs=in_specs, out_specs=out_specs, check_vma=False)
```
